128 devices in a mesh: grp: 4 (over x, y), seq: 32 (over z, core).
Axes of the slice: x: 2, y: 2, z: 16, core: 2. Of those that a mesh axis runs over, the one named last changes fastest.
The devices are a block of a 8x8x16 slice.
Arguments:
- cont_query: bfloat16 [256, 32, 2560], P(('grp', 'seq')), parts along dimension 0, may hold values from -180 to 180
- cont_key: bfloat16 [256, 32, 512], P(('grp', 'seq')), parts along dimension 0, may hold values from -6 to 6
- cont_value: bfloat16 [256, 32, 512], P(('grp', 'seq')), parts along dimension 0, may hold values from -6 to 6
- prefix_key: bfloat16 [16, 2048, 512], P('grp', 'seq'), parts along dimension 0, may hold values from -7 to 7
- prefix_value: bfloat16 [16, 2048, 512], P('grp', 'seq'), parts along dimension 0, may hold values from -6 to 6
- out_weight: bfloat16 [2560, 2560], P(None, 'seq'), may hold values from -0.125 to 0.125
- norm_gain: float32 [2560], replicated, may hold values from 0.5 to 1.5
- lm_head: bfloat16 [2560, 76032], P(None, 'seq'), may hold values from -18 to 18
- target_ids: int32 [256, 32], P(('grp', 'seq')), parts along dimension 0, may hold values from 0 to 76031
- cont_len: int32 [256], P(('grp', 'seq')), parts along dimension 0, may hold values from 8 to 32
- prompt_len: int32 [16], P('grp'), parts along dimension 0, may hold values from 1024 to 2048
- group_of: int32 [256], P('grp'), parts along dimension 0, may hold values from 0 to 3, as said below
- rewards: float32 [256], P(('grp', 'seq')), parts along dimension 0, may hold values from -13 to 13
Outputs:
- token_logprob: float32 [256, 32], P(('grp', 'seq')), parts along dimension 0
- advantage: float32 [256], P(('grp', 'seq')), parts along dimension 0
- objective: float32 [256], P(('grp', 'seq')), parts along dimension 0
The draws below stay inside these ranges and needn't reach their ends.
There are 4 independent parts, one for each index of `grp`. The reference program is written for one: setup_inputs(seed, part) draws one part's arguments, and reference() takes and returns one part's arrays. A program takes and returns all parts, laid end to end along the dimension named above; an argument that names none is the same for every part. Nothing has to cross between parts.
Inputs may be any that keep to these rules, and one draw needn't show every extreme that they name: `group_of`: each of the 4 prompts is named by exactly 16 continuations.
All inputs are finite; a program needn't handle non-finite values.
Results may differ from the reference program's by a relative error of at most 0.0026.
Values may be sent and summed in bfloat16 or wider, within the bound.
A program may use at most 128 MiB of HBM per device.

```python
import math
import jax
import jax.numpy as jnp
import numpy as np
from jax import lax

D = 2560
QH = 20
KVH = 4
HD = 128
VOCAB = 76032
GROUP = 16
CLEN = 32
PROMPT = 2048
CONTS = 64
PROMPTS = 4
N_SEQ = 32


def draw_groups(key):
    shuffled = jax.random.permutation(jax.random.fold_in(key, 11), CONTS)
    return (shuffled // GROUP).astype(jnp.int32)


def draw_group_of(key, part):
    return draw_groups(key)


def draw_prefix_key(key, part):
    drawn = jnp.clip(jax.random.normal(jax.random.fold_in(key, 13), (PROMPTS, PROMPT, KVH * HD), jnp.float32), -6.0, 6.0)
    return drawn.astype(jnp.bfloat16)


def draw_cont_query(key, part):
    drawn = jnp.clip(jax.random.normal(jax.random.fold_in(key, 14), (CONTS, CLEN, QH * HD), jnp.float32), -6.0, 6.0)
    return drawn.astype(jnp.bfloat16)


def draw_lm_head(key, part):
    drawn = jnp.clip(jax.random.normal(jax.random.fold_in(key, 19), (D, VOCAB), jnp.float32), -6.0, 6.0)
    column_scale = jnp.full((1, VOCAB), 3.0 / math.sqrt(D), jnp.float32)
    return (drawn * column_scale).astype(jnp.bfloat16)


def draw_rewards(key, part):
    groups = draw_groups(key)
    spread = jnp.exp(jax.random.uniform(jax.random.fold_in(key, 16), (PROMPTS,), jnp.float32, math.log(0.05), math.log(2.0)))
    offset = jax.random.uniform(jax.random.fold_in(key, 17), (PROMPTS,), jnp.float32, -1.0, 1.0)
    jitter = jnp.clip(jax.random.normal(jax.random.fold_in(key, 18), (CONTS,), jnp.float32), -6.0, 6.0)
    return offset[groups] + spread[groups] * jitter


def place_ends(array, own_key, smallest, largest):
    shape = array.shape
    index_at = [jax.random.randint(jax.random.fold_in(own_key, axis), (), 0, shape[axis]) for axis in range(len(shape))]
    array = array.at[tuple(index_at)].set(smallest)
    longest = shape.index(max(shape))
    index_at[longest] = (index_at[longest] + 1) % shape[longest]
    return array.at[tuple(index_at)].set(largest)


def level_of(stream_key, dims, pieces, least, largest):
    factor_of = 1.0
    for axis_at, blocks in pieces:
        draws = jax.random.uniform(jax.random.fold_in(jax.random.fold_in(stream_key, 6), axis_at), (blocks,), jnp.float32, least / len(pieces), largest / len(pieces))
        factor_of = factor_of * jnp.repeat(jnp.exp(draws), dims[axis_at] // blocks).reshape((-1,) + (1,) * (len(dims) - 1 - axis_at))
    return factor_of


def skewed_wide(stream_key, dims, number_of, lean):
    loads = [min(1 << octave, number_of + 1 - (1 << octave)) * (1 << 20) // math.isqrt((1 << octave) ** lean) + 1 for octave in range((number_of + 1).bit_length()) if 1 << octave <= number_of]
    width = 1 + sum(loads) // (1 << 30)
    listing = np.cumsum(np.array([max(1, weight // width) for weight in loads]))
    ticket = jax.random.randint(jax.random.fold_in(stream_key, 1), dims, 0, int(listing[len(loads) - 1]))
    start = jnp.left_shift(1, jnp.searchsorted(jnp.asarray(listing, jnp.int32), ticket, side="right").astype(jnp.int32))
    grade = start - 1 + jax.random.randint(jax.random.fold_in(stream_key, 4), dims, 0, 1 << 30) % jnp.minimum(start, number_of + 1 - start)
    return jax.random.permutation(jax.random.fold_in(stream_key, 2), number_of)[grade].astype(jnp.int32)


def bell_draw(own_key, shape, scale, bound, shards=(), held_as=jnp.bfloat16):
    values = scale * jax.random.normal(own_key, shape, jnp.float32)
    if shards:
        values = values * level_of(own_key, shape, shards, -0.22, 0.18)
    return jnp.clip(values, -bound, bound).astype(held_as)


def setup_inputs(seed: int = 0, part: int = 0) -> dict:
    key_list = jax.random.split(jax.random.key(seed), 14)
    part_keys = jax.random.split(jax.random.fold_in(key_list[13], part), 14)
    return {
        "cont_query": draw_cont_query(jax.random.fold_in(jax.random.fold_in(key_list[13], part), 71), part),
        "cont_key": bell_draw(part_keys[1], (CONTS, CLEN, KVH * HD), 1.0, 6.0, ((0, 32),)),
        "cont_value": bell_draw(part_keys[2], (CONTS, CLEN, KVH * HD), 1.0, 6.0, ((0, 32),)),
        "prefix_key": draw_prefix_key(jax.random.fold_in(jax.random.fold_in(key_list[13], part), 71), part),
        "prefix_value": bell_draw(part_keys[4], (PROMPTS, PROMPT, KVH * HD), 1.0, 6.0, ((1, 32),)),
        "out_weight": bell_draw(key_list[5], (QH * HD, D), (QH * HD) ** -0.5, 0.125, ((1, 32),)),
        "norm_gain": jnp.clip(1.0 + 0.1 * jax.random.normal(key_list[6], (D,), jnp.float32), 0.5, 1.5),
        "lm_head": draw_lm_head(jax.random.fold_in(key_list[13], 71), part),
        "target_ids": place_ends(skewed_wide(part_keys[8], (CONTS, CLEN), VOCAB, 2), jax.random.fold_in(part_keys[8], 3), 0, VOCAB - 1).astype(jnp.int32),
        "cont_len": place_ends(jax.random.randint(part_keys[9], (CONTS,), CLEN // 4, CLEN + 1), jax.random.fold_in(part_keys[9], 1), CLEN // 4, CLEN).astype(jnp.int32),
        "prompt_len": place_ends(jax.random.randint(part_keys[10], (PROMPTS,), PROMPT // 2, PROMPT + 1), jax.random.fold_in(part_keys[10], 1), PROMPT // 2, PROMPT).astype(jnp.int32),
        "group_of": draw_group_of(jax.random.fold_in(jax.random.fold_in(key_list[13], part), 71), part),
        "rewards": draw_rewards(jax.random.fold_in(jax.random.fold_in(key_list[13], part), 71), part),
    }


NEGATIVE = -1e+30
EPSILON = 1e-06
REWARD_FLOOR = 0.25

def normalize(hidden, norm_gain):
    widened = hidden.astype(jnp.float32)
    factor = lax.rsqrt(lax.optimization_barrier(jnp.mean(widened * widened, axis=-1, keepdims=True)) + EPSILON)
    return (widened * factor * norm_gain).astype(jnp.bfloat16)

def shard_stats(normed, token_ids, head, vocab_offset):
    logits = jnp.dot(normed, head, preferred_element_type=jnp.float32)
    maximum = lax.optimization_barrier(jnp.max(logits, axis=1))
    total_mass = lax.optimization_barrier(jnp.sum(jnp.exp(logits - maximum[:, None]), axis=1))
    columns = vocab_offset + jnp.arange(head.shape[1], dtype=jnp.int32)
    picked = lax.optimization_barrier(jnp.sum(jnp.where(token_ids[:, None] == columns[None, :], logits, 0.0), axis=1))
    return (maximum, total_mass, picked)

def join_stats(first, second):
    maximum = jnp.maximum(first[0], second[0])
    total_mass = first[1] * jnp.exp(first[0] - maximum) + second[1] * jnp.exp(second[0] - maximum)
    return (maximum, total_mass, first[2] + second[2])

def reference(cont_query, cont_key, cont_value, prefix_key, prefix_value, out_weight, norm_gain, lm_head, target_ids, cont_len, prompt_len, group_of, rewards):
    per_group = QH // KVH
    position = jnp.arange(CLEN, dtype=jnp.int32)
    causal = position[None, :] <= position[:, None]
    highest = lax.Precision.HIGHEST

    def attend(index):
        prompt = group_of[index]
        key_rows = jnp.concatenate([prefix_key[prompt], cont_key[index]], axis=0).astype(jnp.float32).reshape(PROMPT + CLEN, KVH, HD)
        value_rows = jnp.concatenate([prefix_value[prompt], cont_value[index]], axis=0).astype(jnp.float32).reshape(PROMPT + CLEN, KVH, HD)
        queries = cont_query[index].astype(jnp.float32).reshape(CLEN, KVH, per_group, HD)
        scores = jnp.einsum('tkgd,skd->tkgs', queries, key_rows, precision=highest) * HD ** (-0.5)
        early = jnp.broadcast_to((jnp.arange(PROMPT, dtype=jnp.int32) < prompt_len[prompt])[None, :], (CLEN, PROMPT))
        visible = jnp.concatenate([early, causal], axis=1)[:, None, None, :]
        scores = jnp.where(visible, scores, NEGATIVE)
        maximum = lax.optimization_barrier(jnp.max(scores, axis=-1, keepdims=True))
        weights = jnp.where(visible, jnp.exp(scores - maximum), 0.0)
        total = lax.optimization_barrier(jnp.sum(weights, axis=-1))
        mixed = jnp.einsum('tkgs,skd->tkgd', weights, value_rows, precision=highest) / total[..., None]
        return mixed.astype(jnp.bfloat16).reshape(CLEN, QH * HD)
    attended = lax.map(attend, jnp.arange(CONTS, dtype=jnp.int32)).reshape(CONTS * CLEN, QH * HD)
    hidden = jnp.dot(attended, out_weight, preferred_element_type=jnp.float32).astype(jnp.bfloat16)
    normed = normalize(hidden, norm_gain)
    token_ids = target_ids.reshape(CONTS * CLEN)
    block = VOCAB // N_SEQ

    def vocab_step(step, running):
        head = lax.dynamic_slice_in_dim(lm_head, step * block, block, 1)
        stats = shard_stats(normed, token_ids, head, step * block)
        return join_stats(running, stats)
    start_stats = (jnp.full((CONTS * CLEN,), NEGATIVE, jnp.float32), jnp.zeros((CONTS * CLEN,), jnp.float32), jnp.zeros((CONTS * CLEN,), jnp.float32))
    maximum, total_mass, picked = lax.fori_loop(0, N_SEQ, vocab_step, start_stats)
    logprob = (picked - maximum - jnp.log(total_mass)).reshape(CONTS, CLEN)
    live = position[None, :] < cont_len[:, None]
    token_logprob = jnp.where(live, logprob, 0.0)
    same_group = (group_of[:, None] == group_of[None, :]).astype(jnp.float32)
    group_mean = jnp.dot(same_group, rewards, precision=highest) / GROUP
    deviation = rewards[None, :] - group_mean[:, None]
    spread = jnp.sqrt(lax.optimization_barrier(jnp.sum(same_group * deviation * deviation, axis=1)) / (GROUP - 1))
    advantage = (rewards - group_mean) / jnp.maximum(spread, REWARD_FLOOR)
    objective = advantage * lax.optimization_barrier(jnp.sum(token_logprob, axis=1)) / cont_len.astype(jnp.float32)
    return (token_logprob, advantage, objective)
```

```python
import functools

import jax
import jax.numpy as jnp
from jax import lax
from jax.experimental import pallas as pl
from jax.experimental.pallas import tpu as pltpu
from jax.sharding import PartitionSpec as P

HD = 128
GROUP = 16
NEGATIVE = -1e30
EPSILON = 1e-06
REWARD_FLOOR = 0.25

CORES = 2
CHUNKS = 4
SKEW = 3
TILE = 480
HALF = 8

BF16 = jnp.bfloat16
F32 = jnp.float32


def dot_last(a, b):
    return lax.dot_general(a, b, (((1,), (1,)), ((), ())), preferred_element_type=F32)


def send(src, dst, send_sem, recv_sem, device):
    return pltpu.make_async_remote_copy(
        src_ref=src,
        dst_ref=dst,
        send_sem=send_sem,
        recv_sem=recv_sem,
        device_id={"seq": device},
        device_id_type=pl.DeviceIdType.MESH,
    )


def kernel(
    dims,
    group_of,
    prompt_len,
    small,
    q,
    ck,
    cv,
    pk,
    pv,
    wt,
    gain,
    lm,
    out,
    kvs,
    kvr,
    qs,
    qr,
    ab,
    hb,
    nt,
    wv,
    gv,
    lv,
    smv,
    smg,
    run_m,
    run_s,
    run_p,
    st,
    sr,
    loc,
    kv_rs,
    kv_rd,
    kv_so,
    kv_sd,
    kv_su,
    kv_sn,
    q_rs,
    q_ss,
    sm_rs,
    sm_ss,
    g_rs,
    g_rd,
    g_sr,
    g_sl,
    g_sd,
    st_rs,
    st_ss,
):
    n, heads, per_head, conts, span, positions = dims
    chips = n // CORES
    side = chips // heads
    vocab = lm.shape[0]
    rows_q = conts * per_head * span
    one_q = per_head * span
    own = conts * span
    feats = wt.shape[0]
    width = per_head * HD
    chunk_rows = n // CHUNKS * own

    me = lax.axis_index("seq")
    z = lax.div(me, CORES)
    co = lax.rem(me, CORES)
    partner = me + 1 - 2 * co
    k0 = lax.div(z, side)
    j = lax.rem(z, side)
    base = k0 * side

    def chip(at):
        return lax.rem(at + chips, chips)

    def dev(at):
        return chip(at) * CORES + co

    def kv_loads(head):
        lanes = pl.ds(pl.multiple_of(head * HD, HD), HD)
        return lanes

    def load_kv(head, carry):
        lanes = kv_loads(head)
        pltpu.make_async_copy(pk.at[:, :, lanes], kvs.at[head, 0], loc.at[0]).start()
        pltpu.make_async_copy(pv.at[:, :, lanes], kvs.at[head, 1], loc.at[0]).start()
        return carry

    lax.fori_loop(0, heads, load_kv, 0)

    def load_q(head, carry):
        for a in range(conts):
            for g in range(per_head):
                lanes = pl.ds(pl.multiple_of((head * per_head + g) * HD, HD), HD)
                pltpu.make_async_copy(
                    q.at[a, :, lanes], qs.at[head, pl.ds(a * one_q + g * span, span), :], loc.at[1]
                ).start()
            lanes = pl.ds(pl.multiple_of(head * HD, HD), HD)
            pltpu.make_async_copy(
                ck.at[a, :, lanes], qs.at[head, pl.ds(rows_q + a * span, span), :], loc.at[1]
            ).start()
            pltpu.make_async_copy(
                cv.at[a, :, lanes], qs.at[head, pl.ds(rows_q + own + a * span, span), :], loc.at[1]
            ).start()
        return carry

    lax.fori_loop(0, heads, load_q, 0)
    pltpu.make_async_copy(small, smv, loc.at[2]).start()

    barrier = pltpu.get_barrier_semaphore()

    def greet(d, carry):
        @pl.when(d != me)
        def _():
            pl.semaphore_signal(
                barrier, inc=1, device_id={"seq": d}, device_id_type=pl.DeviceIdType.MESH
            )

        return carry

    lax.fori_loop(0, n, greet, 0)
    pltpu.make_async_copy(kvs, kvs, loc.at[0]).wait()
    pl.semaphore_wait(barrier, n - 1)

    def kv_at(src):
        rows = pl.ds(pl.multiple_of((chip(src) * CORES + co) * positions, positions), positions)
        return kvr.at[:, :, rows, :]

    def kv_sem(src):
        return chip(src)

    def kv_send(source, head_block, target, send_sem):
        return send(head_block, kv_at(source), send_sem, kv_rs.at[kv_sem(source)], dev(target))

    def kv_d2d(source, block):
        return send(
            block, kv_at(source), kv_sd.at[kv_sem(source)], kv_rd.at[kv_sem(source)], partner
        )

    next_head = lax.rem(k0 + 1, heads)
    prev_head = lax.rem(k0 + heads - 1, heads)
    far_head = lax.rem(k0 + 2, heads)
    own_right = kv_send(z, kvs.at[k0], z + 1, kv_so.at[0])
    own_left = kv_send(z, kvs.at[k0], z - 1, kv_so.at[1])
    ext_right = kv_send(z, kvs.at[next_head], base + side, kv_so.at[2])
    ext_left = kv_send(z, kvs.at[prev_head], base - 1, kv_so.at[3])
    far_right = kv_send(z, kvs.at[far_head], base + 2 * side, kv_so.at[4])
    far_left = kv_send(z, kvs.at[far_head], base - side - 1, kv_so.at[5])
    own_part = kv_d2d(z, kvs.at[k0])

    @pl.when(j >= side // 2)
    def _():
        far_right.start()

    @pl.when(j < side // 2)
    def _():
        far_left.start()

    ext_right.start()
    ext_left.start()

    @pl.when(j < side - 1)
    def _():
        own_right.start()

    @pl.when(j > 0)
    def _():
        own_left.start()

    own_part.start()
    own_rows = pl.ds(pl.multiple_of(me * positions, positions), positions)
    own_lanes = pl.ds(pl.multiple_of(k0 * HD, HD), HD)
    keep_k = pltpu.make_async_copy(pk.at[:, :, own_lanes], kvr.at[0, :, own_rows, :], loc.at[3])
    keep_v = pltpu.make_async_copy(pv.at[:, :, own_lanes], kvr.at[1, :, own_rows, :], loc.at[4])
    keep_k.start()
    keep_v.start()

    pltpu.make_async_copy(qs, qs, loc.at[1]).wait()

    def q_send(step):
        target = chip(z + side * step)
        return send(
            qs.at[lax.div(target, side)],
            qr.at[k0],
            q_ss.at[step],
            q_rs.at[k0],
            dev(target),
        )

    for step in range(1, heads):
        q_send(step).start()

    keep_q = []
    for a in range(conts):
        for g in range(per_head):
            lanes = pl.ds(pl.multiple_of((k0 * per_head + g) * HD, HD), HD)
            keep_q.append((q.at[a, :, lanes], pl.ds(a * one_q + g * span, span)))
        keep_q.append((ck.at[a, :, own_lanes], pl.ds(rows_q + a * span, span)))
        keep_q.append((cv.at[a, :, own_lanes], pl.ds(rows_q + own + a * span, span)))
    for source, rows in keep_q:
        pltpu.make_async_copy(source, qr.at[k0, rows, :], loc.at[5]).start()

    pltpu.make_async_copy(small, smv, loc.at[2]).wait()

    def small_send(d):
        return send(smv, smg.at[me], sm_ss.at[d], sm_rs.at[me], d)

    def small_out(d, carry):
        @pl.when(d != me)
        def _():
            small_send(d).start()

        return carry

    lax.fori_loop(0, n, small_out, 0)
    keep_small = pltpu.make_async_copy(small, smg.at[me], loc.at[2])
    keep_small.start()
    load_w = pltpu.make_async_copy(wt, wv, loc.at[6])
    load_w.start()
    load_gain = pltpu.make_async_copy(gain, gv, loc.at[7])
    load_gain.start()
    load_lm = pltpu.make_async_copy(lm, lv.at[pl.ds(0, vocab), :], loc.at[8])
    load_lm.start()

    reach = side + side // 2

    def up_send(t):
        return kv_send(z - t, kv_at(z - t), z + 1, kv_su.at[t - 1])

    def down_send(t):
        return kv_send(z + t, kv_at(z + t), z - 1, kv_sn.at[t - 1])

    def chain(i, carry):
        t = i + 1

        @pl.when(t <= j + reach)
        def _():
            kv_send(z - t, kv_at(z - t), z + 1, kv_su.at[t - 1]).wait_recv()

            @pl.when(j < side - 1)
            def _():
                up_send(t).start()

            kv_d2d(z - t, kv_at(z - t)).start()

        @pl.when(t <= side - 1 - j + reach)
        def _():
            kv_send(z + t, kv_at(z + t), z - 1, kv_sn.at[t - 1]).wait_recv()

            @pl.when(j > 0)
            def _():
                down_send(t).start()

            kv_d2d(z + t, kv_at(z + t)).start()

        return carry

    longest = side - 1 + reach
    lax.fori_loop(0, longest, chain, 0)

    keep_k.wait()
    keep_v.wait()
    pltpu.make_async_copy(qr.at[k0], qr.at[k0], loc.at[5]).wait()

    def other_rows(src):
        rows = pl.ds(
            pl.multiple_of((src * CORES + 1 - co) * positions, positions), positions
        )
        return kvr.at[:, :, rows, :]

    def kv_partner(src, carry):
        send(other_rows(src), other_rows(src), kv_sd.at[src], kv_rd.at[src], partner).wait_recv()
        return carry

    lax.fori_loop(0, chips, kv_partner, 0)

    def q_arrived(c, carry):
        @pl.when(c != k0)
        def _():
            send(qr.at[c], qr.at[c], q_ss.at[0], q_rs.at[c], partner).wait_recv()

        return carry

    lax.fori_loop(0, heads, q_arrived, 0)

    def block_at(stream, chip_id, core):
        d = chip(chip_id) * CORES + core
        if stream < CHUNKS:
            return ab.at[stream, pl.ds(pl.multiple_of(d * own, own), own), :]
        return hb.at[stream - CHUNKS, pl.ds(pl.multiple_of(d * feats, 16), feats), :]

    def ring_send(stream, source, target, send_sem):
        block = block_at(stream, source, co)
        return send(block, block, send_sem, g_rs.at[stream, chip(source)], dev(target))

    def ring_right(stream, t):
        return ring_send(stream, z - t, z + 1, g_sr.at[stream, t])

    def ring_left(stream, t):
        return ring_send(stream, z + t, z - 1, g_sl.at[stream, t])

    def ring_d2d(stream, source):
        block = block_at(stream, source, co)
        return send(
            block, block, g_sd.at[stream, chip(source)], g_rd.at[stream, chip(source)], partner
        )

    def steps_of(stream):
        right = HALF if stream % 2 == 0 else chips - 1 - HALF
        return right, chips - 1 - right

    def ring_open(stream):
        ring_right(stream, 0).start()
        ring_left(stream, 0).start()
        ring_d2d(stream, z).start()

    def ring_step(stream, t):
        right, left = steps_of(stream)

        @pl.when(t <= right)
        def _():
            ring_send(stream, z - t, z + 1, g_sr.at[stream, 0]).wait_recv()

            @pl.when(t < right)
            def _():
                ring_right(stream, t).start()

        @pl.when(t <= left)
        def _():
            ring_send(stream, z + t, z - 1, g_sl.at[stream, 0]).wait_recv()

            @pl.when(t < left)
            def _():
                ring_left(stream, t).start()

        @pl.when(t <= right)
        def _():
            ring_d2d(stream, z - t).start()

        @pl.when(t <= left)
        def _():
            ring_d2d(stream, z + t).start()

    def ring_partner(stream):
        def arrived(src, carry):
            block = block_at(stream, src, 1 - co)
            send(
                block, block, g_sd.at[stream, src], g_rd.at[stream, src], partner
            ).wait_recv()
            return carry

        lax.fori_loop(0, chips, arrived, 0)

    def attention(c):
        for a in range(conts):
            cont = ((c * side + j) * CORES + co) * conts + a
            g = group_of[cont]
            length = prompt_len[g]
            queries = qr[c, pl.ds(a * one_q, one_q), :]
            own_keys = qr[c, pl.ds(rows_q + a * span, span), :]
            own_values = qr[c, pl.ds(rows_q + own + a * span, span), :]
            scores = dot_last(queries, kvr[0, g]) * HD ** (-0.5)
            at = lax.broadcasted_iota(jnp.int32, scores.shape, 1)
            scores = jnp.where(at < length, scores, NEGATIVE)
            near = dot_last(queries, own_keys) * HD ** (-0.5)
            token = lax.rem(lax.broadcasted_iota(jnp.int32, near.shape, 0), span)
            near = jnp.where(lax.broadcasted_iota(jnp.int32, near.shape, 1) <= token, near, NEGATIVE)
            peak = jnp.maximum(
                jnp.max(scores, axis=1, keepdims=True), jnp.max(near, axis=1, keepdims=True)
            )
            weights = jnp.exp(scores - peak)
            near = jnp.exp(near - peak)
            total = jnp.sum(weights, axis=1, keepdims=True) + jnp.sum(near, axis=1, keepdims=True)
            mixed = jnp.dot(weights.astype(BF16), kvr[1, g], preferred_element_type=F32)
            mixed += jnp.dot(near.astype(BF16), own_values, preferred_element_type=F32)
            mixed = (mixed / total).astype(BF16)
            rows = pl.ds(pl.multiple_of(me * own + a * span, span), span)
            for g5 in range(per_head):
                ab[c, rows, g5 * HD : (g5 + 1) * HD] = mixed[g5 * span : (g5 + 1) * span, :]

    def project(c):
        total = jnp.zeros((feats, chunk_rows), F32)
        for k in range(heads):
            total += dot_last(
                wv[:, k * width : (k + 1) * width], ab[c, pl.ds(k * chunk_rows, chunk_rows), :]
            )
        hb[c, pl.ds(pl.multiple_of(me * feats, 16), feats), :] = total.astype(BF16)

    features = hb.shape[1]
    strip = HD

    def normalize(c):
        def squares(i, total):
            x = hb[c, pl.ds(pl.multiple_of(i * strip, strip), strip), :].astype(F32)
            return total + jnp.sum(x * x, axis=0, keepdims=True)

        total = lax.fori_loop(0, features // strip, squares, jnp.zeros((1, chunk_rows), F32))
        factor = lax.rsqrt(total / features + EPSILON)

        def scale(i, carry):
            rows = pl.ds(pl.multiple_of(i * strip, strip), strip)
            nt[rows, :] = (hb[c, rows, :].astype(F32) * factor * gv[rows, :]).astype(BF16)
            return carry

        lax.fori_loop(0, features // strip, scale, 0)

    def chunk_ids(c):
        rows = []
        for i in range(side):
            d = (c * side + i) * CORES
            rows.append(smg[d, 0:1, :] + smg[d + 1, 0:1, :])
        ids = jnp.concatenate(rows, axis=1).astype(jnp.int32) - me * vocab
        return jnp.where(ids < vocab, ids, -1)

    def tile(c, v):
        rows = pl.ds(pl.multiple_of(v * TILE, 16), TILE)
        logits = jnp.dot(lv[rows, :], nt[...], preferred_element_type=F32)
        at = lax.broadcasted_iota(jnp.int32, logits.shape, 0) + v * TILE
        logits = jnp.where(at < vocab, logits, NEGATIVE)
        run_p[...] += jnp.sum(jnp.where(at == chunk_ids(c), logits, 0.0), axis=0, keepdims=True)
        old = run_m[...]
        new = jnp.maximum(old, jnp.max(logits, axis=0, keepdims=True))
        run_s[...] = run_s[...] * jnp.exp(old - new) + jnp.sum(
            jnp.exp(logits - new), axis=0, keepdims=True
        )
        run_m[...] = new

    def stats_send(c, i, core):
        d = (c * side + i) * CORES + core
        return d, send(st.at[c, i], sr.at[me], st_ss.at[d], st_rs.at[me], d)

    def stats_out(c):
        lse = run_m[...] + jnp.log(run_s[...])
        hit = run_p[...]
        for i in range(side):
            lanes = slice(i * HD, (i + 1) * HD)
            st[c, i, 0:1, :] = lse[:, lanes]
            st[c, i, 1:2, :] = hit[:, lanes]

        @pl.when(k0 == c)
        def _():
            own_lse, own_hit = lse[:, 0:HD], hit[:, 0:HD]
            for i in range(1, side):
                lanes = slice(i * HD, (i + 1) * HD)
                own_lse = jnp.where(j == i, lse[:, lanes], own_lse)
                own_hit = jnp.where(j == i, hit[:, lanes], own_hit)
            sr[me, 0:1, :] = own_lse
            sr[me, 1:2, :] = own_hit

        for i in range(side):
            for core in range(CORES):
                d, copy = stats_send(c, i, core)

                @pl.when(d != me)
                def _(copy=copy):
                    copy.start()

    tiles = -(-vocab // TILE)
    per_slot = -(-(tiles - 1) // (SKEW - 1))

    def slot(i, carry):
        for stream in range(CHUNKS, 2 * CHUNKS):
            t = i - (SKEW * (stream - CHUNKS) + HALF)

            @pl.when(jnp.logical_and(t >= 1, t <= HALF))
            def _(stream=stream, t=t):
                ring_step(stream, t)

        for stream in range(CHUNKS):
            t = i - SKEW * stream

            @pl.when(jnp.logical_and(t >= 1, t <= HALF))
            def _(stream=stream, t=t):
                ring_step(stream, t)

        @pl.when(jnp.logical_and(lax.rem(i, SKEW) == 0, i < SKEW * CHUNKS))
        def _():
            attention(lax.div(i, SKEW))

        for c in range(CHUNKS):

            @pl.when(i == SKEW * c)
            def _(c=c):
                ring_open(c)

        @pl.when(i == HALF)
        def _():
            load_w.wait()

        for c in range(CHUNKS):

            @pl.when(i == SKEW * c + HALF)
            def _(c=c):
                ring_partner(c)
                project(c)
                ring_open(CHUNKS + c)

        m = i - 2 * HALF

        @pl.when(m == 0)
        def _():
            load_gain.wait()
            load_lm.wait()
            keep_small.wait()

            def small_in(d, carry):
                @pl.when(d != me)
                def _():
                    send(smg.at[d], smg.at[d], sm_ss.at[d], sm_rs.at[d], partner).wait_recv()

                return carry

            lax.fori_loop(0, n, small_in, 0)

        for c in range(CHUNKS):

            @pl.when(m == SKEW * c)
            def _(c=c):
                ring_partner(CHUNKS + c)

        @pl.when(m >= 0)
        def _():
            c = lax.div(m, SKEW)
            r = lax.rem(m, SKEW)

            @pl.when(r == 0)
            def _():
                normalize(c)
                run_m[...] = jnp.full_like(run_m, NEGATIVE)
                run_s[...] = jnp.zeros_like(run_s)
                run_p[...] = jnp.zeros_like(run_p)

            first = jnp.maximum(1 + (r - 1) * per_slot, 0)
            first = jnp.where(r == 0, 0, first)
            last = jnp.minimum(1 + r * per_slot, tiles)

            def one(v, carry):
                tile(c, v)
                return carry

            lax.fori_loop(first, last, one, 0)

        for c in range(CHUNKS):

            @pl.when(m == SKEW * c + SKEW - 1)
            def _(c=c):
                stats_out(c)

        return carry

    lax.fori_loop(0, 2 * HALF + SKEW * CHUNKS, slot, 0)

    def stats_in(d, carry):
        @pl.when(d != me)
        def _():
            send(sr.at[d], sr.at[d], st_ss.at[d], st_rs.at[d], partner).wait_recv()

        return carry

    lax.fori_loop(0, n, stats_in, 0)
    everyone = sr[...]
    lse = everyone[:, 0, :]
    peak = jnp.max(lse, axis=0, keepdims=True)
    lse = peak + jnp.log(jnp.sum(jnp.exp(lse - peak), axis=0, keepdims=True))
    out[0:1, :] = jnp.sum(everyone[:, 1, :], axis=0, keepdims=True) - lse
    out[1:2, :] = jnp.sum(smg[...][:, 1, :], axis=0, keepdims=True)

    @pl.when(j >= side // 2)
    def _():
        far_right.wait_send()

    @pl.when(j < side // 2)
    def _():
        far_left.wait_send()

    ext_right.wait_send()
    ext_left.wait_send()

    @pl.when(j < side - 1)
    def _():
        own_right.wait_send()

    @pl.when(j > 0)
    def _():
        own_left.wait_send()

    own_part.wait_send()
    for step in range(1, heads):
        q_send(step).wait_send()

    def chain_out(i, carry):
        t = i + 1

        @pl.when(t <= j + reach)
        def _():
            @pl.when(j < side - 1)
            def _():
                up_send(t).wait_send()

            kv_d2d(z - t, kv_at(z - t)).wait_send()

        @pl.when(t <= side - 1 - j + reach)
        def _():
            @pl.when(j > 0)
            def _():
                down_send(t).wait_send()

            kv_d2d(z + t, kv_at(z + t)).wait_send()

        return carry

    lax.fori_loop(0, longest, chain_out, 0)

    def peers_out(d, carry):
        @pl.when(d != me)
        def _():
            small_send(d).wait_send()
            send(st.at[0, 0], sr.at[me], st_ss.at[d], st_rs.at[me], d).wait_send()

        return carry

    lax.fori_loop(0, n, peers_out, 0)

    def ring_out(t, carry):
        for stream in range(2 * CHUNKS):
            right, left = steps_of(stream)

            @pl.when(t < right)
            def _(stream=stream):
                ring_right(stream, t).wait_send()

            @pl.when(t < left)
            def _(stream=stream):
                ring_left(stream, t).wait_send()

            ring_d2d(stream, t).wait_send()
            ring_d2d(stream, t + HALF).wait_send()
        return carry

    lax.fori_loop(0, HALF, ring_out, 0)


def scores_of(
    n, group_of, prompt_len, small, q, ck, cv, pk, pv, wt, gain, lm
):
    conts, span, query_width = q.shape
    prompts, positions, kv_width = pk.shape
    heads = kv_width // HD
    per_head = query_width // kv_width
    chips = n // CORES
    own = conts * span
    feats, features = wt.shape
    vocab = lm.shape[0]
    chunk_rows = n // CHUNKS * own
    chunk_q = own * per_head + 2 * own
    streams = 2 * CHUNKS
    side = chips // heads
    dims = (n, heads, per_head, conts, span, positions)
    dma = pltpu.SemaphoreType.DMA
    vmem_rows = -(-vocab // TILE) * TILE
    any_spec = pl.BlockSpec(memory_space=pl.ANY)
    smem_spec = pl.BlockSpec(memory_space=pltpu.SMEM)
    return pl.pallas_call(
        functools.partial(kernel, dims),
        out_shape=jax.ShapeDtypeStruct((2, HD), F32),
        in_specs=[smem_spec] * 2 + [any_spec] * 9,
        out_specs=pl.BlockSpec(memory_space=pltpu.VMEM),
        scratch_shapes=[
            pltpu.VMEM((heads, 2, prompts, positions, HD), BF16),
            pltpu.VMEM((2, prompts, n * positions, HD), BF16),
            pltpu.VMEM((heads, chunk_q, HD), BF16),
            pltpu.VMEM((heads, chunk_q, HD), BF16),
            pltpu.VMEM((CHUNKS, n * own, per_head * HD), BF16),
            pltpu.VMEM((CHUNKS, n * feats, chunk_rows), BF16),
            pltpu.VMEM((n * feats, chunk_rows), BF16),
            pltpu.VMEM((feats, features), BF16),
            pltpu.VMEM((n * feats, 1), F32),
            pltpu.VMEM((vmem_rows, n * feats), BF16),
            pltpu.VMEM((2, HD), F32),
            pltpu.VMEM((n, 2, HD), F32),
            pltpu.VMEM((1, chunk_rows), F32),
            pltpu.VMEM((1, chunk_rows), F32),
            pltpu.VMEM((1, chunk_rows), F32),
            pltpu.VMEM((CHUNKS, side, 2, HD), F32),
            pltpu.VMEM((n, 2, HD), F32),
            dma((9,)),
            dma((chips,)),
            dma((chips,)),
            dma((6,)),
            dma((chips,)),
            dma((chips,)),
            dma((chips,)),
            dma((heads,)),
            dma((heads,)),
            dma((n,)),
            dma((n,)),
            dma((streams, chips)),
            dma((streams, chips)),
            dma((streams, HALF)),
            dma((streams, HALF)),
            dma((streams, chips)),
            dma((n,)),
            dma((n,)),
        ],
        compiler_params=pltpu.CompilerParams(
            collective_id=0, has_side_effects=True, vmem_limit_bytes=67_043_328
        ),
        name="scores",
    )(group_of, prompt_len, small, q, ck, cv, pk, pv, wt, gain, lm)


def per_device(
    n,
    cont_query,
    cont_key,
    cont_value,
    prefix_key,
    prefix_value,
    out_weight,
    norm_gain,
    lm_head,
    target_ids,
    cont_len,
    prompt_len,
    group_of,
    rewards,
):
    conts, span, _ = cont_query.shape
    own = conts * span
    me = lax.axis_index("seq")
    co = lax.rem(me, CORES)
    lane = jnp.arange(HD, dtype=jnp.int32)
    ids = jnp.tile(target_ids.reshape(own).astype(F32), CORES)
    ids = jnp.where(lane // own == co, ids, 0.0)
    spread_out = jnp.zeros((HD,), F32)
    for a in range(conts):
        spread_out = jnp.where(lane == me * conts + a, rewards[a], spread_out)
    small = jnp.stack([ids, spread_out])
    found = scores_of(
        n,
        group_of,
        prompt_len,
        small,
        cont_query,
        cont_key,
        cont_value,
        prefix_key,
        prefix_value,
        out_weight.T,
        norm_gain.reshape(-1, 1),
        lm_head.T,
    )
    logprob = lax.dynamic_slice_in_dim(found[0], co * own, own).reshape(conts, span)
    position = jnp.arange(span, dtype=jnp.int32)
    token_logprob = jnp.where(position[None, :] < cont_len[:, None], logprob, 0.0)
    every_reward = found[1, : n * conts]
    own_groups = lax.dynamic_slice_in_dim(group_of, me * conts, conts)
    same = (own_groups[:, None] == group_of[None, :]).astype(F32)
    group_mean = jnp.sum(same * every_reward[None, :], axis=1) / GROUP
    deviation = every_reward[None, :] - group_mean[:, None]
    spread = jnp.sqrt(jnp.sum(same * deviation * deviation, axis=1) / (GROUP - 1))
    advantage = (rewards - group_mean) / jnp.maximum(spread, REWARD_FLOOR)
    objective = advantage * jnp.sum(token_logprob, axis=1) / cont_len.astype(F32)
    return (token_logprob, advantage, objective)


def solution(mesh):
    both = ("grp", "seq")
    in_specs = (
        P(both, None, None),
        P(both, None, None),
        P(both, None, None),
        P("grp", "seq", None),
        P("grp", "seq", None),
        P(None, "seq"),
        P(),
        P(None, "seq"),
        P(both, None),
        P(both),
        P("grp"),
        P("grp"),
        P(both),
    )
    out_specs = (P(both, None), P(both), P(both))
    return jax.shard_map(
        functools.partial(per_device, mesh.shape["seq"]),
        mesh=mesh,
        in_specs=in_specs,
        out_specs=out_specs,
        check_vma=False,
    )
```

```python
import functools

import jax
import jax.numpy as jnp
from jax import lax
from jax.experimental import pallas as pl
from jax.experimental.pallas import tpu as pltpu
from jax.sharding import PartitionSpec as P

HD = 128
GROUP = 16
NEGATIVE = -1e30
EPSILON = 1e-06
REWARD_FLOOR = 0.25

CORES = 2
CHUNKS = 4
SKEW = 2
PER_SLOT = 3
TILE = 480
WEIGH = 160
HALF = 8

BF16 = jnp.bfloat16
F32 = jnp.float32


def dot_last(a, b):
    return lax.dot_general(a, b, (((1,), (1,)), ((), ())), preferred_element_type=F32)


def send(src, dst, send_sem, recv_sem, device):
    return pltpu.make_async_remote_copy(
        src_ref=src,
        dst_ref=dst,
        send_sem=send_sem,
        recv_sem=recv_sem,
        device_id={"seq": device},
        device_id_type=pl.DeviceIdType.MESH,
    )


def kernel(
    dims,
    group_of,
    prompt_len,
    rewards,
    cont_len,
    groups,
    ids,
    gain,
    q,
    ck,
    cv,
    pk,
    pv,
    wt,
    lm,
    out_logprob,
    out_advantage,
    out_objective,
    kvs,
    kvr,
    qs,
    qr,
    ab,
    hb,
    wv,
    lv,
    smv,
    smg,
    run_f,
    run_m,
    run_s,
    run_p,
    st,
    sr,
    loc,
    kv_rs,
    kv_rd,
    kv_so,
    kv_sd,
    kv_su,
    kv_sn,
    q_rs,
    q_ss,
    sm_rs,
    sm_ss,
    g_rs,
    g_rd,
    g_sr,
    g_sl,
    g_sd,
    st_rs,
    st_ss,
):
    n, heads, per_head, conts, span, positions = dims
    chips = n // CORES
    side = chips // heads
    vocab = lm.shape[0]
    rows_q = conts * per_head * span
    one_q = per_head * span
    own = conts * span
    feats = wt.shape[0]
    width = per_head * HD
    chunk_rows = n // CHUNKS * own

    me = lax.axis_index("seq")
    z = lax.div(me, CORES)
    co = lax.rem(me, CORES)
    partner = me + 1 - 2 * co
    k0 = lax.div(z, side)
    j = lax.rem(z, side)
    base = k0 * side

    def chip(at):
        return lax.rem(at + chips, chips)

    def dev(at):
        return chip(at) * CORES + co

    def kv_loads(head):
        lanes = pl.ds(pl.multiple_of(head * HD, HD), HD)
        return lanes

    def load_kv(head, carry):
        lanes = kv_loads(head)
        pltpu.make_async_copy(pk.at[:, :, lanes], kvs.at[head, 0], loc.at[0]).start()
        pltpu.make_async_copy(pv.at[:, :, lanes], kvs.at[head, 1], loc.at[0]).start()
        return carry

    lax.fori_loop(0, heads, load_kv, 0)

    def load_q(head, carry):
        for a in range(conts):
            for g in range(per_head):
                lanes = pl.ds(pl.multiple_of((head * per_head + g) * HD, HD), HD)
                pltpu.make_async_copy(
                    q.at[a, :, lanes], qs.at[head, pl.ds(a * one_q + g * span, span), :], loc.at[1]
                ).start()
            lanes = pl.ds(pl.multiple_of(head * HD, HD), HD)
            pltpu.make_async_copy(
                ck.at[a, :, lanes], qs.at[head, pl.ds(rows_q + a * span, span), :], loc.at[1]
            ).start()
            pltpu.make_async_copy(
                cv.at[a, :, lanes], qs.at[head, pl.ds(rows_q + own + a * span, span), :], loc.at[1]
            ).start()
        return carry

    lax.fori_loop(0, heads, load_q, 0)

    lane = lax.broadcasted_iota(jnp.int32, (1, HD), 1)
    own_ids = ids[...].astype(F32)
    own_ids = jnp.concatenate([own_ids[a : a + 1, :] for a in range(conts)] * CORES, axis=1)
    own_ids = jnp.where(lax.div(lane, own) == co, own_ids, 0.0)
    own_rewards = jnp.zeros((1, HD), F32)
    for a in range(conts):
        own_rewards = jnp.where(lane == me * conts + a, rewards[a], own_rewards)
    smv[0:1, :] = own_ids
    smv[1:2, :] = own_rewards
    smg[me, 0:1, :] = own_ids
    smg[me, 1:2, :] = own_rewards

    barrier = pltpu.get_barrier_semaphore()

    def greet(d, carry):
        @pl.when(d != me)
        def _():
            pl.semaphore_signal(
                barrier, inc=1, device_id={"seq": d}, device_id_type=pl.DeviceIdType.MESH
            )

        return carry

    with jax.named_scope("greet"):
        lax.fori_loop(0, n, greet, 0)
        pltpu.make_async_copy(kvs, kvs, loc.at[0]).wait()
        pl.semaphore_wait(barrier, n - 1)

    def kv_at(src):
        rows = pl.ds(pl.multiple_of((chip(src) * CORES + co) * positions, positions), positions)
        return kvr.at[:, :, rows, :]

    def kv_sem(src):
        return chip(src)

    def kv_send(source, head_block, target, send_sem):
        return send(head_block, kv_at(source), send_sem, kv_rs.at[kv_sem(source)], dev(target))

    def kv_d2d(source, block):
        return send(
            block, kv_at(source), kv_sd.at[kv_sem(source)], kv_rd.at[kv_sem(source)], partner
        )

    next_head = lax.rem(k0 + 1, heads)
    prev_head = lax.rem(k0 + heads - 1, heads)
    far_head = lax.rem(k0 + 2, heads)
    own_right = kv_send(z, kvs.at[k0], z + 1, kv_so.at[0])
    own_left = kv_send(z, kvs.at[k0], z - 1, kv_so.at[1])
    ext_right = kv_send(z, kvs.at[next_head], base + side, kv_so.at[2])
    ext_left = kv_send(z, kvs.at[prev_head], base - 1, kv_so.at[3])
    far_right = kv_send(z, kvs.at[far_head], base + 2 * side, kv_so.at[4])
    far_left = kv_send(z, kvs.at[far_head], base - side - 1, kv_so.at[5])
    own_part = kv_d2d(z, kvs.at[k0])

    @pl.when(j >= side // 2)
    def _():
        far_right.start()

    @pl.when(j < side // 2)
    def _():
        far_left.start()

    ext_right.start()
    ext_left.start()

    @pl.when(j < side - 1)
    def _():
        own_right.start()

    @pl.when(j > 0)
    def _():
        own_left.start()

    own_part.start()
    own_rows = pl.ds(pl.multiple_of(me * positions, positions), positions)
    own_lanes = pl.ds(pl.multiple_of(k0 * HD, HD), HD)
    keep_k = pltpu.make_async_copy(pk.at[:, :, own_lanes], kvr.at[0, :, own_rows, :], loc.at[3])
    keep_v = pltpu.make_async_copy(pv.at[:, :, own_lanes], kvr.at[1, :, own_rows, :], loc.at[4])
    keep_k.start()
    keep_v.start()

    pltpu.make_async_copy(qs, qs, loc.at[1]).wait()

    def q_send(step):
        target = chip(z + side * step)
        if 2 * step == heads:
            shifted = jnp.where(j >= side // 2, side * step - side // 2, side * step + side // 2)
            target = chip(z + shifted)
        return send(
            qs.at[lax.div(target, side)],
            qr.at[k0],
            q_ss.at[step],
            q_rs.at[k0],
            dev(target),
        )

    for step in range(1, heads):
        q_send(step).start()

    keep_q = []
    for a in range(conts):
        for g in range(per_head):
            lanes = pl.ds(pl.multiple_of((k0 * per_head + g) * HD, HD), HD)
            keep_q.append((q.at[a, :, lanes], pl.ds(a * one_q + g * span, span)))
        keep_q.append((ck.at[a, :, own_lanes], pl.ds(rows_q + a * span, span)))
        keep_q.append((cv.at[a, :, own_lanes], pl.ds(rows_q + own + a * span, span)))
    for source, rows in keep_q:
        pltpu.make_async_copy(source, qr.at[k0, rows, :], loc.at[5]).start()


    def small_send(d):
        return send(smv, smg.at[me], sm_ss.at[d], sm_rs.at[me], d)

    def small_out(d, carry):
        @pl.when(d != me)
        def _():
            small_send(d).start()

        return carry

    with jax.named_scope("small"):
        lax.fori_loop(0, n, small_out, 0)
    load_w = pltpu.make_async_copy(wt, wv, loc.at[6])
    load_w.start()
    load_lm = pltpu.make_async_copy(lm, lv.at[pl.ds(0, vocab), :], loc.at[2])
    load_lm.start()

    reach = side + side // 2

    def up_send(t):
        return kv_send(z - t, kv_at(z - t), z + 1, kv_su.at[t - 1])

    def down_send(t):
        return kv_send(z + t, kv_at(z + t), z - 1, kv_sn.at[t - 1])

    def chain(i, carry):
        t = i + 1

        @pl.when(t <= j + reach)
        def _():
            kv_send(z - t, kv_at(z - t), z + 1, kv_su.at[t - 1]).wait_recv()

            @pl.when(j < side - 1)
            def _():
                up_send(t).start()

            kv_d2d(z - t, kv_at(z - t)).start()

        @pl.when(t <= side - 1 - j + reach)
        def _():
            kv_send(z + t, kv_at(z + t), z - 1, kv_sn.at[t - 1]).wait_recv()

            @pl.when(j > 0)
            def _():
                down_send(t).start()

            kv_d2d(z + t, kv_at(z + t)).start()

        return carry

    longest = side - 1 + reach
    with jax.named_scope("chain"):
        lax.fori_loop(0, longest, chain, 0)

    keep_k.wait()
    keep_v.wait()
    pltpu.make_async_copy(qr.at[k0], qr.at[k0], loc.at[5]).wait()

    def other_rows(src):
        rows = pl.ds(
            pl.multiple_of((src * CORES + 1 - co) * positions, positions), positions
        )
        return kvr.at[:, :, rows, :]

    def kv_partner(src, carry):
        send(other_rows(src), other_rows(src), kv_sd.at[src], kv_rd.at[src], partner).wait_recv()
        return carry

    with jax.named_scope("kvpartner"):
        lax.fori_loop(0, chips, kv_partner, 0)

    def q_arrived(c, carry):
        @pl.when(c != k0)
        def _():
            send(qr.at[c], qr.at[c], q_ss.at[0], q_rs.at[c], partner).wait_recv()

        return carry

    with jax.named_scope("qarrive"):
        lax.fori_loop(0, heads, q_arrived, 0)

    def place_of(c, chip_id):
        k = lax.div(chip_id, side)
        away = lax.rem(c - k + heads, heads)
        place = lax.rem(chip_id, side)
        return jnp.where(2 * away == heads, lax.rem(place + side // 2, side), place)

    def token_row(c, chip_id, core):
        k = lax.div(chip_id, side)
        return ((k * side + place_of(c, chip_id)) * CORES + core) * own

    def block_at(stream, chip_id, core):
        d = chip(chip_id) * CORES + core
        if stream < CHUNKS:
            at = token_row(stream, chip(chip_id), core)
            return ab.at[stream, pl.ds(pl.multiple_of(at, own), own), :]
        return hb.at[stream - CHUNKS, pl.ds(pl.multiple_of(d * feats, 16), feats), :]

    def ring_send(stream, source, target, send_sem):
        block = block_at(stream, source, co)
        return send(block, block, send_sem, g_rs.at[stream, chip(source)], dev(target))

    def ring_right(stream, t):
        return ring_send(stream, z - t, z + 1, g_sr.at[stream, t])

    def ring_left(stream, t):
        return ring_send(stream, z + t, z - 1, g_sl.at[stream, t])

    def ring_d2d(stream, source):
        block = block_at(stream, source, co)
        return send(
            block, block, g_sd.at[stream, chip(source)], g_rd.at[stream, chip(source)], partner
        )

    def steps_of(stream):
        right = HALF if stream % 2 == 0 else chips - 1 - HALF
        return right, chips - 1 - right

    def ring_open(stream):
        ring_right(stream, 0).start()
        ring_left(stream, 0).start()
        ring_d2d(stream, z).start()

    def ring_step(stream, t):
        right, left = steps_of(stream)

        @pl.when(t <= right)
        def _():
            ring_send(stream, z - t, z + 1, g_sr.at[stream, 0]).wait_recv()

            @pl.when(t < right)
            def _():
                ring_right(stream, t).start()

        @pl.when(t <= left)
        def _():
            ring_send(stream, z + t, z - 1, g_sl.at[stream, 0]).wait_recv()

            @pl.when(t < left)
            def _():
                ring_left(stream, t).start()

        @pl.when(t <= right)
        def _():
            ring_d2d(stream, z - t).start()

        @pl.when(t <= left)
        def _():
            ring_d2d(stream, z + t).start()

    def ring_partner(stream):
        def arrived(src, carry):
            block = block_at(stream, src, 1 - co)
            send(
                block, block, g_sd.at[stream, src], g_rd.at[stream, src], partner
            ).wait_recv()
            return carry

        lax.fori_loop(0, chips, arrived, 0)

    def attention(c):
        for a in range(conts):
            cont = ((c * side + place_of(c, z)) * CORES + co) * conts + a
            g = group_of[cont]
            length = prompt_len[g]
            queries = qr[c, pl.ds(a * one_q, one_q), :]
            own_keys = qr[c, pl.ds(rows_q + a * span, span), :]
            own_values = qr[c, pl.ds(rows_q + own + a * span, span), :]
            scores = dot_last(queries, kvr[0, g]) * HD ** (-0.5)
            at = lax.broadcasted_iota(jnp.int32, scores.shape, 1)
            scores = jnp.where(at < length, scores, NEGATIVE)
            near = dot_last(queries, own_keys) * HD ** (-0.5)
            token = lax.rem(lax.broadcasted_iota(jnp.int32, near.shape, 0), span)
            near = jnp.where(lax.broadcasted_iota(jnp.int32, near.shape, 1) <= token, near, NEGATIVE)
            peak = jnp.maximum(
                jnp.max(scores, axis=1, keepdims=True), jnp.max(near, axis=1, keepdims=True)
            )
            weights = jnp.exp(scores - peak)
            near = jnp.exp(near - peak)
            total = jnp.sum(weights, axis=1, keepdims=True) + jnp.sum(near, axis=1, keepdims=True)
            mixed = jnp.dot(weights.astype(BF16), kvr[1, g], preferred_element_type=F32)
            mixed += jnp.dot(near.astype(BF16), own_values, preferred_element_type=F32)
            mixed = (mixed / total).astype(BF16)
            rows = pl.ds(pl.multiple_of(token_row(c, z, co) + a * span, span), span)
            for g5 in range(per_head):
                ab[c, rows, g5 * HD : (g5 + 1) * HD] = mixed[g5 * span : (g5 + 1) * span, :]

    def project(c):
        total = jnp.zeros((feats, chunk_rows), F32)
        for k in range(heads):
            total += dot_last(
                wv[:, k * width : (k + 1) * width], ab[c, pl.ds(k * chunk_rows, chunk_rows), :]
            )
        hb[c, pl.ds(pl.multiple_of(me * feats, 16), feats), :] = total.astype(BF16)

    features = hb.shape[1]
    strip = HD

    def normalize(c):
        def squares(i, total):
            x = hb[c, pl.ds(pl.multiple_of(i * strip, strip), strip), :].astype(F32)
            return total + jnp.sum(x * x, axis=0, keepdims=True)

        total = lax.fori_loop(0, features // strip, squares, jnp.zeros((1, chunk_rows), F32))
        run_f[...] = lax.rsqrt(total / features + EPSILON)

    def weigh(i):
        rows = pl.ds(pl.multiple_of(i * WEIGH, 16), WEIGH)
        lv[rows, :] = (lv[rows, :].astype(F32) * gain[...]).astype(BF16)

    def chunk_ids(c):
        rows = []
        for i in range(side):
            d = (c * side + i) * CORES
            rows.append(smg[d, 0:1, :] + smg[d + 1, 0:1, :])
        ids = jnp.concatenate(rows, axis=1).astype(jnp.int32) - me * vocab
        return jnp.where(ids < vocab, ids, -1)

    def tile(c, v):
        rows = pl.ds(pl.multiple_of(v * TILE, 16), TILE)
        logits = jnp.dot(lv[rows, :], hb[c], preferred_element_type=F32) * run_f[...]
        at = lax.broadcasted_iota(jnp.int32, logits.shape, 0) + v * TILE
        logits = jnp.where(at < vocab, logits, NEGATIVE)
        run_p[...] += jnp.sum(jnp.where(at == chunk_ids(c), logits, 0.0), axis=0, keepdims=True)
        old = run_m[...]
        new = jnp.maximum(old, jnp.max(logits, axis=0, keepdims=True))
        run_s[...] = run_s[...] * jnp.exp(old - new) + jnp.sum(
            jnp.exp(logits - new), axis=0, keepdims=True
        )
        run_m[...] = new

    def stats_send(c, i, core):
        d = (c * side + i) * CORES + core
        return d, send(st.at[c, i], sr.at[me], st_ss.at[d], st_rs.at[me], d)

    def stats_out(c):
        lse = run_m[...] + jnp.log(run_s[...])
        hit = run_p[...]
        for i in range(side):
            lanes = slice(i * HD, (i + 1) * HD)
            st[c, i, 0:1, :] = lse[:, lanes]
            st[c, i, 1:2, :] = hit[:, lanes]

        @pl.when(k0 == c)
        def _():
            own_lse, own_hit = lse[:, 0:HD], hit[:, 0:HD]
            for i in range(1, side):
                lanes = slice(i * HD, (i + 1) * HD)
                own_lse = jnp.where(j == i, lse[:, lanes], own_lse)
                own_hit = jnp.where(j == i, hit[:, lanes], own_hit)
            sr[me, 0:1, :] = own_lse
            sr[me, 1:2, :] = own_hit

        for i in range(side):
            for core in range(CORES):
                d, copy = stats_send(c, i, core)

                @pl.when(d != me)
                def _(copy=copy):
                    copy.start()

    tiles = -(-vocab // TILE)
    steps = []
    finished = 0
    while finished < tiles * CHUNKS:
        at = len(steps)
        steps.append(finished)
        ready = sum(at >= 2 * HALF + SKEW * c for c in range(CHUNKS)) * tiles
        finished = min(finished + PER_SLOT, ready)
    slots = len(steps)
    steps.append(finished)

    def slot(i, carry):
        for stream in range(CHUNKS, 2 * CHUNKS):
            t = i - (SKEW * (stream - CHUNKS) + HALF)

            @pl.when(jnp.logical_and(t >= 1, t <= HALF))
            def _(stream=stream, t=t):
                with jax.named_scope(f"hid{stream}"):
                    ring_step(stream, t)

        for stream in range(CHUNKS):
            t = i - SKEW * stream

            @pl.when(jnp.logical_and(t >= 1, t <= HALF))
            def _(stream=stream, t=t):
                with jax.named_scope(f"att{stream}"):
                    ring_step(stream, t)

        @pl.when(jnp.logical_and(lax.rem(i, SKEW) == 0, i < SKEW * CHUNKS))
        def _():
            with jax.named_scope("attention"):
                attention(lax.div(i, SKEW))

        for c in range(CHUNKS):

            @pl.when(i == SKEW * c)
            def _(c=c):
                ring_open(c)

        @pl.when(i == HALF)
        def _():
            load_w.wait()

        @pl.when(i == 0)
        def _():
            load_lm.wait()

        @pl.when(i < lv.shape[0] // WEIGH)
        def _():
            with jax.named_scope("weigh"):
                weigh(i)

        for c in range(CHUNKS):

            @pl.when(i == SKEW * c + HALF)
            def _(c=c):
                with jax.named_scope("partner1"):
                    ring_partner(c)
                with jax.named_scope("project"):
                    project(c)
                ring_open(CHUNKS + c)

        m = i - 2 * HALF

        @pl.when(m == 0)
        def _():
            def small_in(d, carry):
                @pl.when(d != me)
                def _():
                    send(smg.at[d], smg.at[d], sm_ss.at[d], sm_rs.at[d], partner).wait_recv()

                return carry

            lax.fori_loop(0, n, small_in, 0)

        for c in range(CHUNKS):

            @pl.when(m == SKEW * c)
            def _(c=c):
                with jax.named_scope("partner2"):
                    ring_partner(CHUNKS + c)

        first = 0
        last = 0
        for at in range(2 * HALF, slots):
            first = first + jnp.where(i > at, steps[at + 1] - steps[at], 0)
            last = last + jnp.where(i >= at, steps[at + 1] - steps[at], 0)

        def one(step, carry):
            c = lax.div(step, tiles)
            v = lax.rem(step, tiles)

            @pl.when(v == 0)
            def _():
                with jax.named_scope("norm"):
                    normalize(c)
                run_m[...] = jnp.full_like(run_m, NEGATIVE)
                run_s[...] = jnp.zeros_like(run_s)
                run_p[...] = jnp.zeros_like(run_p)

            with jax.named_scope("tile"):
                tile(c, v)

            @pl.when(v == tiles - 1)
            def _():
                with jax.named_scope("stats"):
                    stats_out(c)

            return carry

        lax.fori_loop(first, last, one, 0)
        return carry

    with jax.named_scope("slots"):
        lax.fori_loop(0, slots, slot, 0)

    every_reward = jnp.sum(smg[...][:, 1, :], axis=0, keepdims=True)[:, 0 : n * conts]
    advantages = []
    for a in range(conts):
        same = groups[...] == group_of[me * conts + a]
        mean = jnp.sum(jnp.where(same, every_reward, 0.0), axis=1, keepdims=True) / GROUP
        off = every_reward - mean
        spread = jnp.sum(jnp.where(same, off * off, 0.0), axis=1, keepdims=True)
        spread = jnp.sqrt(spread / (GROUP - 1))
        advantages.append((rewards[a] - mean) / jnp.maximum(spread, REWARD_FLOOR))

    def stats_in(d, carry):
        @pl.when(d != me)
        def _():
            send(sr.at[d], sr.at[d], st_ss.at[d], st_rs.at[d], partner).wait_recv()

        return carry

    with jax.named_scope("join"):
        lax.fori_loop(0, n, stats_in, 0)
    everyone = sr[...]
    lse = everyone[:, 0, :]
    peak = jnp.max(lse, axis=0, keepdims=True)
    lse = peak + jnp.log(jnp.sum(jnp.exp(lse - peak), axis=0, keepdims=True))
    logprob = jnp.sum(everyone[:, 1, :], axis=0, keepdims=True) - lse
    logprob = jnp.where(co == 0, logprob[:, 0:own], logprob[:, own : 2 * own])
    position = lax.broadcasted_iota(jnp.int32, (1, span), 1)
    for a in range(conts):
        live = jnp.where(position < cont_len[a], logprob[:, a * span : (a + 1) * span], 0.0)
        out_logprob[a : a + 1, :] = live
        gained = advantages[a] * jnp.sum(live, axis=1, keepdims=True)
        gained = gained / jnp.full((1, 1), cont_len[a], jnp.int32).astype(F32)
        out_advantage[a] = advantages[a][0, 0]
        out_objective[a] = gained[0, 0]

    @pl.when(j >= side // 2)
    def _():
        far_right.wait_send()

    @pl.when(j < side // 2)
    def _():
        far_left.wait_send()

    ext_right.wait_send()
    ext_left.wait_send()

    @pl.when(j < side - 1)
    def _():
        own_right.wait_send()

    @pl.when(j > 0)
    def _():
        own_left.wait_send()

    own_part.wait_send()
    for step in range(1, heads):
        q_send(step).wait_send()

    def chain_out(i, carry):
        t = i + 1

        @pl.when(t <= j + reach)
        def _():
            @pl.when(j < side - 1)
            def _():
                up_send(t).wait_send()

            kv_d2d(z - t, kv_at(z - t)).wait_send()

        @pl.when(t <= side - 1 - j + reach)
        def _():
            @pl.when(j > 0)
            def _():
                down_send(t).wait_send()

            kv_d2d(z + t, kv_at(z + t)).wait_send()

        return carry

    lax.fori_loop(0, longest, chain_out, 0)

    def peers_out(d, carry):
        @pl.when(d != me)
        def _():
            small_send(d).wait_send()
            send(st.at[0, 0], sr.at[me], st_ss.at[d], st_rs.at[me], d).wait_send()

        return carry

    lax.fori_loop(0, n, peers_out, 0)

    def ring_out(t, carry):
        for stream in range(2 * CHUNKS):
            right, left = steps_of(stream)

            @pl.when(t < right)
            def _(stream=stream):
                ring_right(stream, t).wait_send()

            @pl.when(t < left)
            def _(stream=stream):
                ring_left(stream, t).wait_send()

            ring_d2d(stream, t).wait_send()
            ring_d2d(stream, t + HALF).wait_send()
        return carry

    lax.fori_loop(0, HALF, ring_out, 0)


def scores_of(
    n, group_of, prompt_len, rewards, cont_len, groups, ids, gain, q, ck, cv, pk, pv, wt, lm
):
    conts, span, query_width = q.shape
    prompts, positions, kv_width = pk.shape
    heads = kv_width // HD
    per_head = query_width // kv_width
    chips = n // CORES
    own = conts * span
    feats, features = wt.shape
    vocab = lm.shape[0]
    chunk_rows = n // CHUNKS * own
    chunk_q = own * per_head + 2 * own
    streams = 2 * CHUNKS
    side = chips // heads
    dims = (n, heads, per_head, conts, span, positions)
    dma = pltpu.SemaphoreType.DMA
    vmem_rows = -(-vocab // TILE) * TILE
    any_spec = pl.BlockSpec(memory_space=pl.ANY)
    smem_spec = pl.BlockSpec(memory_space=pltpu.SMEM)
    vmem_spec = pl.BlockSpec(memory_space=pltpu.VMEM)
    return pl.pallas_call(
        functools.partial(kernel, dims),
        out_shape=(
            jax.ShapeDtypeStruct((conts, span), F32),
            jax.ShapeDtypeStruct((conts,), F32),
            jax.ShapeDtypeStruct((conts,), F32),
        ),
        in_specs=[smem_spec] * 4 + [vmem_spec] * 3 + [any_spec] * 7,
        out_specs=(vmem_spec, smem_spec, smem_spec),
        scratch_shapes=[
            pltpu.VMEM((heads, 2, prompts, positions, HD), BF16),
            pltpu.VMEM((2, prompts, n * positions, HD), BF16),
            pltpu.VMEM((heads, chunk_q, HD), BF16),
            pltpu.VMEM((heads, chunk_q, HD), BF16),
            pltpu.VMEM((CHUNKS, n * own, per_head * HD), BF16),
            pltpu.VMEM((CHUNKS, n * feats, chunk_rows), BF16),
            pltpu.VMEM((feats, features), BF16),
            pltpu.VMEM((vmem_rows, n * feats), BF16),
            pltpu.VMEM((2, HD), F32),
            pltpu.VMEM((n, 2, HD), F32),
            pltpu.VMEM((1, chunk_rows), F32),
            pltpu.VMEM((1, chunk_rows), F32),
            pltpu.VMEM((1, chunk_rows), F32),
            pltpu.VMEM((1, chunk_rows), F32),
            pltpu.VMEM((CHUNKS, side, 2, HD), F32),
            pltpu.VMEM((n, 2, HD), F32),
            dma((9,)),
            dma((chips,)),
            dma((chips,)),
            dma((6,)),
            dma((chips,)),
            dma((chips,)),
            dma((chips,)),
            dma((heads,)),
            dma((heads,)),
            dma((n,)),
            dma((n,)),
            dma((streams, chips)),
            dma((streams, chips)),
            dma((streams, HALF)),
            dma((streams, HALF)),
            dma((streams, chips)),
            dma((n,)),
            dma((n,)),
        ],
        compiler_params=pltpu.CompilerParams(
            collective_id=0, has_side_effects=True, vmem_limit_bytes=67_043_328
        ),
        name="scores",
    )(group_of, prompt_len, rewards, cont_len, groups, ids, gain, q, ck, cv, pk, pv, wt, lm)


def per_device(
    n,
    cont_query,
    cont_key,
    cont_value,
    prefix_key,
    prefix_value,
    out_weight,
    norm_gain,
    lm_head,
    target_ids,
    cont_len,
    prompt_len,
    group_of,
    rewards,
):
    return scores_of(
        n,
        group_of,
        prompt_len,
        rewards,
        cont_len,
        group_of.reshape(1, -1),
        target_ids,
        norm_gain.reshape(1, -1),
        cont_query,
        cont_key,
        cont_value,
        prefix_key,
        prefix_value,
        out_weight.T,
        lm_head.T,
    )


def solution(mesh):
    both = ("grp", "seq")
    in_specs = (
        P(both, None, None),
        P(both, None, None),
        P(both, None, None),
        P("grp", "seq", None),
        P("grp", "seq", None),
        P(None, "seq"),
        P(),
        P(None, "seq"),
        P(both, None),
        P(both),
        P("grp"),
        P("grp"),
        P(both),
    )
    out_specs = (P(both, None), P(both), P(both))
    return jax.shard_map(
        functools.partial(per_device, mesh.shape["seq"]),
        mesh=mesh,
        in_specs=in_specs,
        out_specs=out_specs,
        check_vma=False,
    )
```

```python
import functools

import jax
import jax.numpy as jnp
from jax import lax
from jax.experimental import pallas as pl
from jax.experimental.pallas import tpu as pltpu
from jax.sharding import PartitionSpec as P

HD = 128
GROUP = 16
NEGATIVE = -1e30
EPSILON = 1e-06
REWARD_FLOOR = 0.25

Q_AT = (0, 3, 5, 3)
CORES = 2
CHUNKS = 4
STARTS = (0, 0, 5, 7)
PER_SLOT = 2
TILE = 480
WEIGH = 160
HALF = 8

BF16 = jnp.bfloat16
F32 = jnp.float32


def dot_last(a, b):
    return lax.dot_general(a, b, (((1,), (1,)), ((), ())), preferred_element_type=F32)


def send(src, dst, send_sem, recv_sem, device):
    return pltpu.make_async_remote_copy(
        src_ref=src,
        dst_ref=dst,
        send_sem=send_sem,
        recv_sem=recv_sem,
        device_id={"seq": device},
        device_id_type=pl.DeviceIdType.MESH,
    )


def kernel(
    dims,
    group_of,
    prompt_len,
    rewards,
    cont_len,
    groups,
    ids,
    gain,
    q,
    ck,
    cv,
    pk,
    pv,
    wt,
    lm,
    out_logprob,
    out_advantage,
    out_objective,
    kvs,
    kvr,
    qs,
    qr,
    ab,
    hb,
    wv,
    lv,
    smv,
    smg,
    run_f,
    run_m,
    run_s,
    run_p,
    st,
    sr,
    loc,
    kv_rs,
    kv_rd,
    kv_so,
    kv_sd,
    kv_su,
    kv_sn,
    q_rs,
    q_ss,
    sm_rs,
    sm_ss,
    g_rs,
    g_rd,
    g_sr,
    g_sl,
    g_sd,
    st_rs,
    st_ss,
):
    n, heads, per_head, conts, span, positions = dims
    chips = n // CORES
    side = chips // heads
    vocab = lm.shape[0]
    rows_q = conts * per_head * span
    one_q = per_head * span
    own = conts * span
    feats = wt.shape[0]
    width = per_head * HD
    chunk_rows = n // CHUNKS * own

    me = lax.axis_index("seq")
    z = lax.div(me, CORES)
    co = lax.rem(me, CORES)
    partner = me + 1 - 2 * co
    k0 = lax.div(z, side)
    j = lax.rem(z, side)
    base = k0 * side

    def chip(at):
        return lax.rem(at + chips, chips)

    def dev(at):
        return chip(at) * CORES + co

    def kv_loads(head):
        lanes = pl.ds(pl.multiple_of(head * HD, HD), HD)
        return lanes

    def load_kv(head, carry):
        lanes = kv_loads(head)
        pltpu.make_async_copy(pk.at[:, :, lanes], kvs.at[head, 0], loc.at[0]).start()
        pltpu.make_async_copy(pv.at[:, :, lanes], kvs.at[head, 1], loc.at[0]).start()
        return carry

    lax.fori_loop(0, heads, load_kv, 0)

    def load_q(head, carry):
        for a in range(conts):
            for g in range(per_head):
                lanes = pl.ds(pl.multiple_of((head * per_head + g) * HD, HD), HD)
                pltpu.make_async_copy(
                    q.at[a, :, lanes], qs.at[head, pl.ds(a * one_q + g * span, span), :], loc.at[1]
                ).start()
            lanes = pl.ds(pl.multiple_of(head * HD, HD), HD)
            pltpu.make_async_copy(
                ck.at[a, :, lanes], qs.at[head, pl.ds(rows_q + a * span, span), :], loc.at[1]
            ).start()
            pltpu.make_async_copy(
                cv.at[a, :, lanes], qs.at[head, pl.ds(rows_q + own + a * span, span), :], loc.at[1]
            ).start()
        return carry

    lax.fori_loop(0, heads, load_q, 0)

    lane = lax.broadcasted_iota(jnp.int32, (1, HD), 1)
    own_ids = ids[...].astype(F32)
    own_ids = jnp.concatenate([own_ids[a : a + 1, :] for a in range(conts)] * CORES, axis=1)
    own_ids = jnp.where(lax.div(lane, own) == co, own_ids, 0.0)
    own_rewards = jnp.zeros((1, HD), F32)
    for a in range(conts):
        own_rewards = jnp.where(lane == me * conts + a, rewards[a], own_rewards)
    smv[0:1, :] = own_ids
    smv[1:2, :] = own_rewards
    smg[me, 0:1, :] = own_ids
    smg[me, 1:2, :] = own_rewards

    barrier = pltpu.get_barrier_semaphore()

    def greet(d, carry):
        @pl.when(d != me)
        def _():
            pl.semaphore_signal(
                barrier, inc=1, device_id={"seq": d}, device_id_type=pl.DeviceIdType.MESH
            )

        return carry

    with jax.named_scope("greet"):
        lax.fori_loop(0, n, greet, 0)
        pltpu.make_async_copy(kvs, kvs, loc.at[0]).wait()
        pl.semaphore_wait(barrier, n - 1)

    def kv_at(src):
        rows = pl.ds(pl.multiple_of((chip(src) * CORES + co) * positions, positions), positions)
        return kvr.at[:, :, rows, :]

    def kv_sem(src):
        return chip(src)

    def kv_send(source, head_block, target, send_sem):
        return send(head_block, kv_at(source), send_sem, kv_rs.at[kv_sem(source)], dev(target))

    def kv_d2d(source, block):
        return send(
            block, kv_at(source), kv_sd.at[kv_sem(source)], kv_rd.at[kv_sem(source)], partner
        )

    next_head = lax.rem(k0 + 1, heads)
    prev_head = lax.rem(k0 + heads - 1, heads)
    far_head = lax.rem(k0 + 2, heads)
    own_right = kv_send(z, kvs.at[k0], z + 1, kv_so.at[0])
    own_left = kv_send(z, kvs.at[k0], z - 1, kv_so.at[1])
    ext_right = kv_send(z, kvs.at[next_head], base + side, kv_so.at[2])
    ext_left = kv_send(z, kvs.at[prev_head], base - 1, kv_so.at[3])
    far_right = kv_send(z, kvs.at[far_head], base + 2 * side, kv_so.at[4])
    far_left = kv_send(z, kvs.at[far_head], base - side - 1, kv_so.at[5])
    own_part = kv_d2d(z, kvs.at[k0])

    @pl.when(j < side - 1)
    def _():
        own_right.start()

    @pl.when(j > 0)
    def _():
        own_left.start()

    own_part.start()
    own_rows = pl.ds(pl.multiple_of(me * positions, positions), positions)
    own_lanes = pl.ds(pl.multiple_of(k0 * HD, HD), HD)
    keep_k = pltpu.make_async_copy(pk.at[:, :, own_lanes], kvr.at[0, :, own_rows, :], loc.at[3])
    keep_v = pltpu.make_async_copy(pv.at[:, :, own_lanes], kvr.at[1, :, own_rows, :], loc.at[4])
    keep_k.start()
    keep_v.start()

    pltpu.make_async_copy(qs, qs, loc.at[1]).wait()

    def q_send(step):
        target = chip(z + side * step)
        if 2 * step == heads:
            shifted = jnp.where(j >= side // 2, side * step - side // 2, side * step + side // 2)
            target = chip(z + shifted)
        return send(
            qs.at[lax.div(target, side)],
            qr.at[k0],
            q_ss.at[step],
            q_rs.at[k0],
            dev(target),
        )

    keep_q = []
    for a in range(conts):
        for g in range(per_head):
            lanes = pl.ds(pl.multiple_of((k0 * per_head + g) * HD, HD), HD)
            keep_q.append((q.at[a, :, lanes], pl.ds(a * one_q + g * span, span)))
        keep_q.append((ck.at[a, :, own_lanes], pl.ds(rows_q + a * span, span)))
        keep_q.append((cv.at[a, :, own_lanes], pl.ds(rows_q + own + a * span, span)))
    for source, rows in keep_q:
        pltpu.make_async_copy(source, qr.at[k0, rows, :], loc.at[5]).start()


    def small_send(d):
        return send(smv, smg.at[me], sm_ss.at[d], sm_rs.at[me], d)

    def small_out(d, carry):
        @pl.when(d != me)
        def _():
            small_send(d).start()

        return carry

    with jax.named_scope("small"):
        lax.fori_loop(0, n, small_out, 0)
    load_w = pltpu.make_async_copy(wt, wv, loc.at[6])
    load_w.start()
    load_lm = pltpu.make_async_copy(lm, lv.at[pl.ds(0, vocab), :], loc.at[2])
    load_lm.start()

    reach = side + side // 2

    def up_send(t):
        return kv_send(z - t, kv_at(z - t), z + 1, kv_su.at[t - 1])

    def down_send(t):
        return kv_send(z + t, kv_at(z + t), z - 1, kv_sn.at[t - 1])

    def depart(i):
        @pl.when(i == side - 1 - j)
        def _():
            ext_right.start()

        @pl.when(i == j)
        def _():
            ext_left.start()

        @pl.when(jnp.logical_and(j >= side // 2, i == 2 * (side - 1) - j))
        def _():
            far_right.start()

        @pl.when(jnp.logical_and(j < side // 2, i == side - 1 + j))
        def _():
            far_left.start()

        for step in range(1, heads):

            @pl.when(i == Q_AT[step])
            def _(step=step):
                q_send(step).start()

    def chain(i, carry):
        t = i + 1
        depart(i)

        @pl.when(t <= j + reach)
        def _():
            kv_send(z - t, kv_at(z - t), z + 1, kv_su.at[t - 1]).wait_recv()

            @pl.when(j < side - 1)
            def _():
                up_send(t).start()

            kv_d2d(z - t, kv_at(z - t)).start()

        @pl.when(t <= side - 1 - j + reach)
        def _():
            kv_send(z + t, kv_at(z + t), z - 1, kv_sn.at[t - 1]).wait_recv()

            @pl.when(j > 0)
            def _():
                down_send(t).start()

            kv_d2d(z + t, kv_at(z + t)).start()

        return carry

    longest = side - 1 + reach
    with jax.named_scope("chain"):
        lax.fori_loop(0, longest, chain, 0)

    keep_k.wait()
    keep_v.wait()
    pltpu.make_async_copy(qr.at[k0], qr.at[k0], loc.at[5]).wait()

    def other_rows(src):
        rows = pl.ds(
            pl.multiple_of((src * CORES + 1 - co) * positions, positions), positions
        )
        return kvr.at[:, :, rows, :]

    def kv_partner(src, carry):
        send(other_rows(src), other_rows(src), kv_sd.at[src], kv_rd.at[src], partner).wait_recv()
        return carry

    with jax.named_scope("kvpartner"):
        lax.fori_loop(0, chips, kv_partner, 0)

    def q_arrived(c, carry):
        @pl.when(c != k0)
        def _():
            send(qr.at[c], qr.at[c], q_ss.at[0], q_rs.at[c], partner).wait_recv()

        return carry

    with jax.named_scope("qarrive"):
        lax.fori_loop(0, heads, q_arrived, 0)

    def place_of(c, chip_id):
        k = lax.div(chip_id, side)
        away = lax.rem(c - k + heads, heads)
        place = lax.rem(chip_id, side)
        return jnp.where(2 * away == heads, lax.rem(place + side // 2, side), place)

    def token_row(c, chip_id, core):
        k = lax.div(chip_id, side)
        return ((k * side + place_of(c, chip_id)) * CORES + core) * own

    def block_at(stream, chip_id, core):
        d = chip(chip_id) * CORES + core
        if stream < CHUNKS:
            at = token_row(stream, chip(chip_id), core)
            return ab.at[stream, pl.ds(pl.multiple_of(at, own), own), :]
        return hb.at[stream - CHUNKS, pl.ds(pl.multiple_of(d * feats, 16), feats), :]

    def ring_send(stream, source, target, send_sem):
        block = block_at(stream, source, co)
        return send(block, block, send_sem, g_rs.at[stream, chip(source)], dev(target))

    def ring_right(stream, t):
        return ring_send(stream, z - t, z + 1, g_sr.at[stream, t])

    def ring_left(stream, t):
        return ring_send(stream, z + t, z - 1, g_sl.at[stream, t])

    def ring_d2d(stream, source):
        block = block_at(stream, source, co)
        return send(
            block, block, g_sd.at[stream, chip(source)], g_rd.at[stream, chip(source)], partner
        )

    def steps_of(stream):
        right = HALF if stream % 2 == 0 else chips - 1 - HALF
        return right, chips - 1 - right

    def ring_open(stream):
        ring_right(stream, 0).start()
        ring_left(stream, 0).start()
        ring_d2d(stream, z).start()

    def attended_open(c):
        rows = pl.ds(pl.multiple_of(token_row(c, z, co), own), own)
        block = ab.at[c, rows, :]
        send(block, block, g_sr.at[c, 0], g_rs.at[c, z], dev(z + 1)).start()
        send(block, block, g_sl.at[c, 0], g_rs.at[c, z], dev(z - 1)).start()
        send(block, block, g_sd.at[c, z], g_rd.at[c, z], partner).start()

    def ring_step(stream, t):
        right, left = steps_of(stream)

        @pl.when(t <= right)
        def _():
            ring_send(stream, z - t, z + 1, g_sr.at[stream, 0]).wait_recv()

            @pl.when(t < right)
            def _():
                ring_right(stream, t).start()

        @pl.when(t <= left)
        def _():
            ring_send(stream, z + t, z - 1, g_sl.at[stream, 0]).wait_recv()

            @pl.when(t < left)
            def _():
                ring_left(stream, t).start()

        @pl.when(t <= right)
        def _():
            ring_d2d(stream, z - t).start()

        @pl.when(t <= left)
        def _():
            ring_d2d(stream, z + t).start()

    def ring_partner(stream):
        def arrived(src, carry):
            block = block_at(stream, src, 1 - co)
            send(
                block, block, g_sd.at[stream, src], g_rd.at[stream, src], partner
            ).wait_recv()
            return carry

        lax.fori_loop(0, chips, arrived, 0)

    def attention(c):
        for a in range(conts):
            cont = ((c * side + place_of(c, z)) * CORES + co) * conts + a
            g = group_of[cont]
            length = prompt_len[g]
            queries = qr[c, pl.ds(a * one_q, one_q), :]
            own_keys = qr[c, pl.ds(rows_q + a * span, span), :]
            own_values = qr[c, pl.ds(rows_q + own + a * span, span), :]
            scores = dot_last(queries, kvr[0, g]) * HD ** (-0.5)
            at = lax.broadcasted_iota(jnp.int32, scores.shape, 1)
            scores = jnp.where(at < length, scores, NEGATIVE)
            near = dot_last(queries, own_keys) * HD ** (-0.5)
            token = lax.rem(lax.broadcasted_iota(jnp.int32, near.shape, 0), span)
            near = jnp.where(lax.broadcasted_iota(jnp.int32, near.shape, 1) <= token, near, NEGATIVE)
            peak = jnp.maximum(
                jnp.max(scores, axis=1, keepdims=True), jnp.max(near, axis=1, keepdims=True)
            )
            weights = jnp.exp(scores - peak)
            near = jnp.exp(near - peak)
            total = jnp.sum(weights, axis=1, keepdims=True) + jnp.sum(near, axis=1, keepdims=True)
            mixed = jnp.dot(weights.astype(BF16), kvr[1, g], preferred_element_type=F32)
            mixed += jnp.dot(near.astype(BF16), own_values, preferred_element_type=F32)
            mixed = (mixed / total).astype(BF16)
            rows = pl.ds(pl.multiple_of(token_row(c, z, co) + a * span, span), span)
            for g5 in range(per_head):
                ab[c, rows, g5 * HD : (g5 + 1) * HD] = mixed[g5 * span : (g5 + 1) * span, :]

    def project(c):
        total = jnp.zeros((feats, chunk_rows), F32)
        for k in range(heads):
            total += dot_last(
                wv[:, k * width : (k + 1) * width], ab[c, pl.ds(k * chunk_rows, chunk_rows), :]
            )
        hb[c, pl.ds(pl.multiple_of(me * feats, 16), feats), :] = total.astype(BF16)

    features = hb.shape[1]
    strip = HD

    def normalize(c):
        def squares(i, total):
            x = hb[c, pl.ds(pl.multiple_of(i * strip, strip), strip), :].astype(F32)
            return total + jnp.sum(x * x, axis=0, keepdims=True)

        total = lax.fori_loop(0, features // strip, squares, jnp.zeros((1, chunk_rows), F32))
        run_f[...] = lax.rsqrt(total / features + EPSILON)

    def weigh(i):
        rows = pl.ds(pl.multiple_of(i * WEIGH, 16), WEIGH)
        lv[rows, :] = (lv[rows, :].astype(F32) * gain[...]).astype(BF16)

    def chunk_ids(c):
        rows = []
        for i in range(side):
            d = (c * side + i) * CORES
            rows.append(smg[d, 0:1, :] + smg[d + 1, 0:1, :])
        ids = jnp.concatenate(rows, axis=1).astype(jnp.int32) - me * vocab
        return jnp.where(ids < vocab, ids, -1)

    def tile(c, v):
        rows = pl.ds(pl.multiple_of(v * TILE, 16), TILE)
        logits = jnp.dot(lv[rows, :], hb[c], preferred_element_type=F32) * run_f[...]
        at = lax.broadcasted_iota(jnp.int32, logits.shape, 0) + v * TILE
        logits = jnp.where(at < vocab, logits, NEGATIVE)
        run_p[...] += jnp.sum(jnp.where(at == chunk_ids(c), logits, 0.0), axis=0, keepdims=True)
        old = run_m[...]
        new = jnp.maximum(old, jnp.max(logits, axis=0, keepdims=True))
        run_s[...] = run_s[...] * jnp.exp(old - new) + jnp.sum(
            jnp.exp(logits - new), axis=0, keepdims=True
        )
        run_m[...] = new

    def stats_send(c, i, core):
        d = (c * side + i) * CORES + core
        return d, send(st.at[c, i], sr.at[me], st_ss.at[d], st_rs.at[me], d)

    def stats_out(c):
        lse = run_m[...] + jnp.log(run_s[...])
        hit = run_p[...]
        for i in range(side):
            lanes = slice(i * HD, (i + 1) * HD)
            st[c, i, 0:1, :] = lse[:, lanes]
            st[c, i, 1:2, :] = hit[:, lanes]

        @pl.when(k0 == c)
        def _():
            own_lse, own_hit = lse[:, 0:HD], hit[:, 0:HD]
            for i in range(1, side):
                lanes = slice(i * HD, (i + 1) * HD)
                own_lse = jnp.where(j == i, lse[:, lanes], own_lse)
                own_hit = jnp.where(j == i, hit[:, lanes], own_hit)
            sr[me, 0:1, :] = own_lse
            sr[me, 1:2, :] = own_hit

        for i in range(side):
            for core in range(CORES):
                d, copy = stats_send(c, i, core)

                @pl.when(d != me)
                def _(copy=copy):
                    copy.start()

    tiles = -(-vocab // TILE)
    steps = []
    finished = 0
    while finished < tiles * CHUNKS:
        at = len(steps)
        steps.append(finished)
        ready = sum(at >= 2 * HALF + start for start in STARTS) * tiles
        finished = min(finished + PER_SLOT, ready)
    slots = len(steps)
    steps.append(finished)

    def slot(i, carry):
        for stream in range(CHUNKS, 2 * CHUNKS):
            t = i - (STARTS[stream - CHUNKS] + HALF)

            @pl.when(jnp.logical_and(t >= 1, t <= HALF))
            def _(stream=stream, t=t):
                with jax.named_scope(f"hid{stream}"):
                    ring_step(stream, t)

        for stream in range(CHUNKS):
            t = i - STARTS[stream]

            @pl.when(jnp.logical_and(t >= 1, t <= HALF))
            def _(stream=stream, t=t):
                with jax.named_scope(f"att{stream}"):
                    ring_step(stream, t)

        def begin(c, carry):
            with jax.named_scope("attention"):
                attention(c)
            attended_open(c)
            return carry

        begun = sum((i > start).astype(jnp.int32) for start in STARTS)
        due = sum((i >= start).astype(jnp.int32) for start in STARTS)
        lax.fori_loop(begun, due, begin, 0)

        @pl.when(i == HALF)
        def _():
            load_w.wait()

        @pl.when(i == 0)
        def _():
            load_lm.wait()

        @pl.when(i < lv.shape[0] // WEIGH)
        def _():
            with jax.named_scope("weigh"):
                weigh(i)

        for c in range(CHUNKS):

            @pl.when(i == STARTS[c] + HALF)
            def _(c=c):
                with jax.named_scope("partner1"):
                    ring_partner(c)
                with jax.named_scope("project"):
                    project(c)
                ring_open(CHUNKS + c)

        m = i - 2 * HALF

        @pl.when(m == 0)
        def _():
            def small_in(d, carry):
                @pl.when(d != me)
                def _():
                    send(smg.at[d], smg.at[d], sm_ss.at[d], sm_rs.at[d], partner).wait_recv()

                return carry

            lax.fori_loop(0, n, small_in, 0)

        for c in range(CHUNKS):

            @pl.when(m == STARTS[c])
            def _(c=c):
                with jax.named_scope("partner2"):
                    ring_partner(CHUNKS + c)

        first = 0
        last = 0
        for at in range(2 * HALF, slots):
            first = first + jnp.where(i > at, steps[at + 1] - steps[at], 0)
            last = last + jnp.where(i >= at, steps[at + 1] - steps[at], 0)

        def one(step, carry):
            c = lax.div(step, tiles)
            v = lax.rem(step, tiles)

            @pl.when(v == 0)
            def _():
                with jax.named_scope("norm"):
                    normalize(c)
                run_m[...] = jnp.full_like(run_m, NEGATIVE)
                run_s[...] = jnp.zeros_like(run_s)
                run_p[...] = jnp.zeros_like(run_p)

            with jax.named_scope("tile"):
                tile(c, v)

            @pl.when(v == tiles - 1)
            def _():
                with jax.named_scope("stats"):
                    stats_out(c)

            return carry

        lax.fori_loop(first, last, one, 0)
        return carry

    with jax.named_scope("slots"):
        lax.fori_loop(0, slots, slot, 0)

    every_reward = jnp.sum(smg[...][:, 1, :], axis=0, keepdims=True)[:, 0 : n * conts]
    advantages = []
    for a in range(conts):
        same = groups[...] == group_of[me * conts + a]
        mean = jnp.sum(jnp.where(same, every_reward, 0.0), axis=1, keepdims=True) / GROUP
        off = every_reward - mean
        spread = jnp.sum(jnp.where(same, off * off, 0.0), axis=1, keepdims=True)
        spread = jnp.sqrt(spread / (GROUP - 1))
        advantages.append((rewards[a] - mean) / jnp.maximum(spread, REWARD_FLOOR))

    def stats_in(d, carry):
        @pl.when(d != me)
        def _():
            send(sr.at[d], sr.at[d], st_ss.at[d], st_rs.at[d], partner).wait_recv()

        return carry

    with jax.named_scope("join"):
        lax.fori_loop(0, n, stats_in, 0)
    everyone = sr[...]
    lse = everyone[:, 0, :]
    peak = jnp.max(lse, axis=0, keepdims=True)
    lse = peak + jnp.log(jnp.sum(jnp.exp(lse - peak), axis=0, keepdims=True))
    logprob = jnp.sum(everyone[:, 1, :], axis=0, keepdims=True) - lse
    logprob = jnp.where(co == 0, logprob[:, 0:own], logprob[:, own : 2 * own])
    position = lax.broadcasted_iota(jnp.int32, (1, span), 1)
    for a in range(conts):
        live = jnp.where(position < cont_len[a], logprob[:, a * span : (a + 1) * span], 0.0)
        out_logprob[a : a + 1, :] = live
        gained = advantages[a] * jnp.sum(live, axis=1, keepdims=True)
        gained = gained / jnp.full((1, 1), cont_len[a], jnp.int32).astype(F32)
        out_advantage[a] = advantages[a][0, 0]
        out_objective[a] = gained[0, 0]

    @pl.when(j >= side // 2)
    def _():
        far_right.wait_send()

    @pl.when(j < side // 2)
    def _():
        far_left.wait_send()

    ext_right.wait_send()
    ext_left.wait_send()

    @pl.when(j < side - 1)
    def _():
        own_right.wait_send()

    @pl.when(j > 0)
    def _():
        own_left.wait_send()

    own_part.wait_send()
    for step in range(1, heads):
        q_send(step).wait_send()

    def chain_out(i, carry):
        t = i + 1

        @pl.when(t <= j + reach)
        def _():
            @pl.when(j < side - 1)
            def _():
                up_send(t).wait_send()

            kv_d2d(z - t, kv_at(z - t)).wait_send()

        @pl.when(t <= side - 1 - j + reach)
        def _():
            @pl.when(j > 0)
            def _():
                down_send(t).wait_send()

            kv_d2d(z + t, kv_at(z + t)).wait_send()

        return carry

    lax.fori_loop(0, longest, chain_out, 0)

    def peers_out(d, carry):
        @pl.when(d != me)
        def _():
            small_send(d).wait_send()
            send(st.at[0, 0], sr.at[me], st_ss.at[d], st_rs.at[me], d).wait_send()

        return carry

    lax.fori_loop(0, n, peers_out, 0)

    def ring_out(t, carry):
        for stream in range(2 * CHUNKS):
            right, left = steps_of(stream)

            @pl.when(t < right)
            def _(stream=stream):
                ring_right(stream, t).wait_send()

            @pl.when(t < left)
            def _(stream=stream):
                ring_left(stream, t).wait_send()

            ring_d2d(stream, t).wait_send()
            ring_d2d(stream, t + HALF).wait_send()
        return carry

    lax.fori_loop(0, HALF, ring_out, 0)


def scores_of(
    n, group_of, prompt_len, rewards, cont_len, groups, ids, gain, q, ck, cv, pk, pv, wt, lm
):
    conts, span, query_width = q.shape
    prompts, positions, kv_width = pk.shape
    heads = kv_width // HD
    per_head = query_width // kv_width
    chips = n // CORES
    own = conts * span
    feats, features = wt.shape
    vocab = lm.shape[0]
    chunk_rows = n // CHUNKS * own
    chunk_q = own * per_head + 2 * own
    streams = 2 * CHUNKS
    side = chips // heads
    dims = (n, heads, per_head, conts, span, positions)
    dma = pltpu.SemaphoreType.DMA
    vmem_rows = -(-vocab // TILE) * TILE
    any_spec = pl.BlockSpec(memory_space=pl.ANY)
    smem_spec = pl.BlockSpec(memory_space=pltpu.SMEM)
    vmem_spec = pl.BlockSpec(memory_space=pltpu.VMEM)
    return pl.pallas_call(
        functools.partial(kernel, dims),
        out_shape=(
            jax.ShapeDtypeStruct((conts, span), F32),
            jax.ShapeDtypeStruct((conts,), F32),
            jax.ShapeDtypeStruct((conts,), F32),
        ),
        in_specs=[smem_spec] * 4 + [vmem_spec] * 3 + [any_spec] * 7,
        out_specs=(vmem_spec, smem_spec, smem_spec),
        scratch_shapes=[
            pltpu.VMEM((heads, 2, prompts, positions, HD), BF16),
            pltpu.VMEM((2, prompts, n * positions, HD), BF16),
            pltpu.VMEM((heads, chunk_q, HD), BF16),
            pltpu.VMEM((heads, chunk_q, HD), BF16),
            pltpu.VMEM((CHUNKS, n * own, per_head * HD), BF16),
            pltpu.VMEM((CHUNKS, n * feats, chunk_rows), BF16),
            pltpu.VMEM((feats, features), BF16),
            pltpu.VMEM((vmem_rows, n * feats), BF16),
            pltpu.VMEM((2, HD), F32),
            pltpu.VMEM((n, 2, HD), F32),
            pltpu.VMEM((1, chunk_rows), F32),
            pltpu.VMEM((1, chunk_rows), F32),
            pltpu.VMEM((1, chunk_rows), F32),
            pltpu.VMEM((1, chunk_rows), F32),
            pltpu.VMEM((CHUNKS, side, 2, HD), F32),
            pltpu.VMEM((n, 2, HD), F32),
            dma((9,)),
            dma((chips,)),
            dma((chips,)),
            dma((6,)),
            dma((chips,)),
            dma((chips,)),
            dma((chips,)),
            dma((heads,)),
            dma((heads,)),
            dma((n,)),
            dma((n,)),
            dma((streams, chips)),
            dma((streams, chips)),
            dma((streams, HALF)),
            dma((streams, HALF)),
            dma((streams, chips)),
            dma((n,)),
            dma((n,)),
        ],
        compiler_params=pltpu.CompilerParams(
            collective_id=0, has_side_effects=True, vmem_limit_bytes=67_043_328
        ),
        name="scores",
    )(group_of, prompt_len, rewards, cont_len, groups, ids, gain, q, ck, cv, pk, pv, wt, lm)


def per_device(
    n,
    cont_query,
    cont_key,
    cont_value,
    prefix_key,
    prefix_value,
    out_weight,
    norm_gain,
    lm_head,
    target_ids,
    cont_len,
    prompt_len,
    group_of,
    rewards,
):
    return scores_of(
        n,
        group_of,
        prompt_len,
        rewards,
        cont_len,
        group_of.reshape(1, -1),
        target_ids,
        norm_gain.reshape(1, -1),
        cont_query,
        cont_key,
        cont_value,
        prefix_key,
        prefix_value,
        out_weight.T,
        lm_head.T,
    )


def solution(mesh):
    both = ("grp", "seq")
    in_specs = (
        P(both, None, None),
        P(both, None, None),
        P(both, None, None),
        P("grp", "seq", None),
        P("grp", "seq", None),
        P(None, "seq"),
        P(),
        P(None, "seq"),
        P(both, None),
        P(both),
        P("grp"),
        P("grp"),
        P(both),
    )
    out_specs = (P(both, None), P(both), P(both))
    return jax.shard_map(
        functools.partial(per_device, mesh.shape["seq"]),
        mesh=mesh,
        in_specs=in_specs,
        out_specs=out_specs,
        check_vma=False,
    )
```

```python
import functools

import jax
import jax.numpy as jnp
from jax import lax
from jax.experimental import pallas as pl
from jax.experimental.pallas import tpu as pltpu
from jax.sharding import PartitionSpec as P

HD = 128
GROUP = 16
NEGATIVE = -1e30
EPSILON = 1e-06
REWARD_FLOOR = 0.25

Q_AT = (0, 3, 5, 3)
CORES = 2
CHUNKS = 4
STARTS = (0, 0, 5, 7)
PER_SLOT = 2
TILE = 480
PIECES = 3
WEIGH = 160
HALF = 8

BF16 = jnp.bfloat16
F32 = jnp.float32


def dot_last(a, b):
    return lax.dot_general(a, b, (((1,), (1,)), ((), ())), preferred_element_type=F32)


def send(src, dst, send_sem, recv_sem, device):
    return pltpu.make_async_remote_copy(
        src_ref=src,
        dst_ref=dst,
        send_sem=send_sem,
        recv_sem=recv_sem,
        device_id={"seq": device},
        device_id_type=pl.DeviceIdType.MESH,
    )


def kernel(
    dims,
    group_of,
    prompt_len,
    rewards,
    cont_len,
    groups,
    ids,
    gain,
    q,
    ck,
    cv,
    pk,
    pv,
    wt,
    lm,
    out_logprob,
    out_advantage,
    out_objective,
    kvs,
    kvr,
    qs,
    qr,
    ab,
    hb,
    wv,
    lv,
    smv,
    smg,
    run_f,
    run_m,
    run_s,
    run_p,
    st,
    sr,
    loc,
    kv_rs,
    kv_rd,
    kv_so,
    kv_sd,
    kv_su,
    kv_sn,
    q_rs,
    q_ss,
    sm_rs,
    sm_ss,
    g_rs,
    g_rd,
    g_sr,
    g_sl,
    g_sd,
    st_rs,
    st_ss,
):
    n, heads, per_head, conts, span, positions = dims
    chips = n // CORES
    side = chips // heads
    vocab = lm.shape[0]
    rows_q = conts * per_head * span
    one_q = per_head * span
    own = conts * span
    feats = wt.shape[0]
    width = per_head * HD
    chunk_rows = n // CHUNKS * own

    me = lax.axis_index("seq")
    z = lax.div(me, CORES)
    co = lax.rem(me, CORES)
    partner = me + 1 - 2 * co
    k0 = lax.div(z, side)
    j = lax.rem(z, side)
    base = k0 * side

    def chip(at):
        return lax.rem(at + chips, chips)

    def dev(at):
        return chip(at) * CORES + co

    def kv_loads(head):
        lanes = pl.ds(pl.multiple_of(head * HD, HD), HD)
        return lanes

    def load_kv(head, carry):
        lanes = kv_loads(head)
        pltpu.make_async_copy(pk.at[:, :, lanes], kvs.at[head, 0], loc.at[0]).start()
        pltpu.make_async_copy(pv.at[:, :, lanes], kvs.at[head, 1], loc.at[0]).start()
        return carry

    lax.fori_loop(0, heads, load_kv, 0)

    def load_q(head, carry):
        for a in range(conts):
            for g in range(per_head):
                lanes = pl.ds(pl.multiple_of((head * per_head + g) * HD, HD), HD)
                pltpu.make_async_copy(
                    q.at[a, :, lanes], qs.at[head, pl.ds(a * one_q + g * span, span), :], loc.at[1]
                ).start()
            lanes = pl.ds(pl.multiple_of(head * HD, HD), HD)
            pltpu.make_async_copy(
                ck.at[a, :, lanes], qs.at[head, pl.ds(rows_q + a * span, span), :], loc.at[1]
            ).start()
            pltpu.make_async_copy(
                cv.at[a, :, lanes], qs.at[head, pl.ds(rows_q + own + a * span, span), :], loc.at[1]
            ).start()
        return carry

    lax.fori_loop(0, heads, load_q, 0)

    lane = lax.broadcasted_iota(jnp.int32, (1, HD), 1)
    own_ids = ids[...].astype(F32)
    own_ids = jnp.concatenate([own_ids[a : a + 1, :] for a in range(conts)] * CORES, axis=1)
    own_ids = jnp.where(lax.div(lane, own) == co, own_ids, 0.0)
    own_rewards = jnp.zeros((1, HD), F32)
    for a in range(conts):
        own_rewards = jnp.where(lane == me * conts + a, rewards[a], own_rewards)
    smv[0:1, :] = own_ids
    smv[1:2, :] = own_rewards
    smg[me, 0:1, :] = own_ids
    smg[me, 1:2, :] = own_rewards

    barrier = pltpu.get_barrier_semaphore()

    def greet(d, carry):
        @pl.when(d != me)
        def _():
            pl.semaphore_signal(
                barrier, inc=1, device_id={"seq": d}, device_id_type=pl.DeviceIdType.MESH
            )

        return carry

    with jax.named_scope("greet"):
        lax.fori_loop(0, n, greet, 0)
        pltpu.make_async_copy(kvs, kvs, loc.at[0]).wait()
        pl.semaphore_wait(barrier, n - 1)

    def kv_at(src):
        rows = pl.ds(pl.multiple_of((chip(src) * CORES + co) * positions, positions), positions)
        return kvr.at[:, :, rows, :]

    def kv_sem(src):
        return chip(src)

    def kv_send(source, head_block, target, send_sem):
        return send(head_block, kv_at(source), send_sem, kv_rs.at[kv_sem(source)], dev(target))

    def kv_d2d(source, block):
        return send(
            block, kv_at(source), kv_sd.at[kv_sem(source)], kv_rd.at[kv_sem(source)], partner
        )

    next_head = lax.rem(k0 + 1, heads)
    prev_head = lax.rem(k0 + heads - 1, heads)
    far_head = lax.rem(k0 + 2, heads)
    own_right = kv_send(z, kvs.at[k0], z + 1, kv_so.at[0])
    own_left = kv_send(z, kvs.at[k0], z - 1, kv_so.at[1])
    ext_right = kv_send(z, kvs.at[next_head], base + side, kv_so.at[2])
    ext_left = kv_send(z, kvs.at[prev_head], base - 1, kv_so.at[3])
    far_right = kv_send(z, kvs.at[far_head], base + 2 * side, kv_so.at[4])
    far_left = kv_send(z, kvs.at[far_head], base - side - 1, kv_so.at[5])
    own_part = kv_d2d(z, kvs.at[k0])

    @pl.when(j < side - 1)
    def _():
        own_right.start()

    @pl.when(j > 0)
    def _():
        own_left.start()

    own_part.start()
    own_rows = pl.ds(pl.multiple_of(me * positions, positions), positions)
    own_lanes = pl.ds(pl.multiple_of(k0 * HD, HD), HD)
    keep_k = pltpu.make_async_copy(pk.at[:, :, own_lanes], kvr.at[0, :, own_rows, :], loc.at[3])
    keep_v = pltpu.make_async_copy(pv.at[:, :, own_lanes], kvr.at[1, :, own_rows, :], loc.at[4])
    keep_k.start()
    keep_v.start()

    pltpu.make_async_copy(qs, qs, loc.at[1]).wait()

    def q_send(step):
        target = chip(z + side * step)
        if 2 * step == heads:
            shifted = jnp.where(j >= side // 2, side * step - side // 2, side * step + side // 2)
            target = chip(z + shifted)
        return send(
            qs.at[lax.div(target, side)],
            qr.at[k0],
            q_ss.at[step],
            q_rs.at[k0],
            dev(target),
        )

    keep_q = []
    for a in range(conts):
        for g in range(per_head):
            lanes = pl.ds(pl.multiple_of((k0 * per_head + g) * HD, HD), HD)
            keep_q.append((q.at[a, :, lanes], pl.ds(a * one_q + g * span, span)))
        keep_q.append((ck.at[a, :, own_lanes], pl.ds(rows_q + a * span, span)))
        keep_q.append((cv.at[a, :, own_lanes], pl.ds(rows_q + own + a * span, span)))
    for source, rows in keep_q:
        pltpu.make_async_copy(source, qr.at[k0, rows, :], loc.at[5]).start()


    def small_send(d):
        return send(smv, smg.at[me], sm_ss.at[d], sm_rs.at[me], d)

    def small_out(d, carry):
        @pl.when(d != me)
        def _():
            small_send(d).start()

        return carry

    with jax.named_scope("small"):
        lax.fori_loop(0, n, small_out, 0)
    load_w = pltpu.make_async_copy(wt, wv, loc.at[6])
    load_w.start()
    load_lm = pltpu.make_async_copy(lm, lv.at[pl.ds(0, vocab), :], loc.at[2])
    load_lm.start()

    reach = side + side // 2

    def up_send(t):
        return kv_send(z - t, kv_at(z - t), z + 1, kv_su.at[t - 1])

    def down_send(t):
        return kv_send(z + t, kv_at(z + t), z - 1, kv_sn.at[t - 1])

    def depart(i):
        @pl.when(i == side - 1 - j)
        def _():
            ext_right.start()

        @pl.when(i == j)
        def _():
            ext_left.start()

        @pl.when(jnp.logical_and(j >= side // 2, i == 2 * (side - 1) - j))
        def _():
            far_right.start()

        @pl.when(jnp.logical_and(j < side // 2, i == side - 1 + j))
        def _():
            far_left.start()

        for step in range(1, heads):

            @pl.when(i == Q_AT[step])
            def _(step=step):
                q_send(step).start()

    def chain(i, carry):
        t = i + 1
        depart(i)

        @pl.when(t <= j + reach)
        def _():
            kv_send(z - t, kv_at(z - t), z + 1, kv_su.at[t - 1]).wait_recv()

            @pl.when(j < side - 1)
            def _():
                up_send(t).start()

            kv_d2d(z - t, kv_at(z - t)).start()

        @pl.when(t <= side - 1 - j + reach)
        def _():
            kv_send(z + t, kv_at(z + t), z - 1, kv_sn.at[t - 1]).wait_recv()

            @pl.when(j > 0)
            def _():
                down_send(t).start()

            kv_d2d(z + t, kv_at(z + t)).start()

        return carry

    longest = side - 1 + reach
    with jax.named_scope("chain"):
        lax.fori_loop(0, longest, chain, 0)

    keep_k.wait()
    keep_v.wait()
    pltpu.make_async_copy(qr.at[k0], qr.at[k0], loc.at[5]).wait()

    def other_rows(src):
        rows = pl.ds(
            pl.multiple_of((src * CORES + 1 - co) * positions, positions), positions
        )
        return kvr.at[:, :, rows, :]

    def kv_partner(src, carry):
        send(other_rows(src), other_rows(src), kv_sd.at[src], kv_rd.at[src], partner).wait_recv()
        return carry

    with jax.named_scope("kvpartner"):
        lax.fori_loop(0, chips, kv_partner, 0)

    def q_arrived(c, carry):
        @pl.when(c != k0)
        def _():
            send(qr.at[c], qr.at[c], q_ss.at[0], q_rs.at[c], partner).wait_recv()

        return carry

    with jax.named_scope("qarrive"):
        lax.fori_loop(0, heads, q_arrived, 0)

    def place_of(c, chip_id):
        k = lax.div(chip_id, side)
        away = lax.rem(c - k + heads, heads)
        place = lax.rem(chip_id, side)
        return jnp.where(2 * away == heads, lax.rem(place + side // 2, side), place)

    def token_row(c, chip_id, core):
        k = lax.div(chip_id, side)
        return ((k * side + place_of(c, chip_id)) * CORES + core) * own

    def block_at(stream, chip_id, core):
        d = chip(chip_id) * CORES + core
        if stream < CHUNKS:
            at = token_row(stream, chip(chip_id), core)
            return ab.at[stream, pl.ds(pl.multiple_of(at, own), own), :]
        return hb.at[stream - CHUNKS, pl.ds(pl.multiple_of(d * feats, 16), feats), :]

    def ring_send(stream, source, target, send_sem):
        block = block_at(stream, source, co)
        return send(block, block, send_sem, g_rs.at[stream, chip(source)], dev(target))

    def ring_right(stream, t):
        return ring_send(stream, z - t, z + 1, g_sr.at[stream, t])

    def ring_left(stream, t):
        return ring_send(stream, z + t, z - 1, g_sl.at[stream, t])

    def ring_d2d(stream, source):
        block = block_at(stream, source, co)
        return send(
            block, block, g_sd.at[stream, chip(source)], g_rd.at[stream, chip(source)], partner
        )

    def steps_of(stream):
        right = HALF if stream % 2 == 0 else chips - 1 - HALF
        return right, chips - 1 - right

    def ring_open(stream):
        ring_right(stream, 0).start()
        ring_left(stream, 0).start()
        ring_d2d(stream, z).start()

    def attended_open(c):
        rows = pl.ds(pl.multiple_of(token_row(c, z, co), own), own)
        block = ab.at[c, rows, :]
        send(block, block, g_sr.at[c, 0], g_rs.at[c, z], dev(z + 1)).start()
        send(block, block, g_sl.at[c, 0], g_rs.at[c, z], dev(z - 1)).start()
        send(block, block, g_sd.at[c, z], g_rd.at[c, z], partner).start()

    def ring_step(stream, t):
        right, left = steps_of(stream)

        @pl.when(t <= right)
        def _():
            ring_send(stream, z - t, z + 1, g_sr.at[stream, 0]).wait_recv()

            @pl.when(t < right)
            def _():
                ring_right(stream, t).start()

        @pl.when(t <= left)
        def _():
            ring_send(stream, z + t, z - 1, g_sl.at[stream, 0]).wait_recv()

            @pl.when(t < left)
            def _():
                ring_left(stream, t).start()

        @pl.when(t <= right)
        def _():
            ring_d2d(stream, z - t).start()

        @pl.when(t <= left)
        def _():
            ring_d2d(stream, z + t).start()

    def ring_partner(stream):
        def arrived(src, carry):
            block = block_at(stream, src, 1 - co)
            send(
                block, block, g_sd.at[stream, src], g_rd.at[stream, src], partner
            ).wait_recv()
            return carry

        lax.fori_loop(0, chips, arrived, 0)

    def attention(c):
        for a in range(conts):
            cont = ((c * side + place_of(c, z)) * CORES + co) * conts + a
            g = group_of[cont]
            length = prompt_len[g]
            queries = qr[c, pl.ds(a * one_q, one_q), :]
            own_keys = qr[c, pl.ds(rows_q + a * span, span), :]
            own_values = qr[c, pl.ds(rows_q + own + a * span, span), :]
            scores = dot_last(queries, kvr[0, g]) * HD ** (-0.5)
            at = lax.broadcasted_iota(jnp.int32, scores.shape, 1)
            scores = jnp.where(at < length, scores, NEGATIVE)
            near = dot_last(queries, own_keys) * HD ** (-0.5)
            token = lax.rem(lax.broadcasted_iota(jnp.int32, near.shape, 0), span)
            near = jnp.where(lax.broadcasted_iota(jnp.int32, near.shape, 1) <= token, near, NEGATIVE)
            peak = jnp.maximum(
                jnp.max(scores, axis=1, keepdims=True), jnp.max(near, axis=1, keepdims=True)
            )
            weights = jnp.exp(scores - peak)
            near = jnp.exp(near - peak)
            total = jnp.sum(weights, axis=1, keepdims=True) + jnp.sum(near, axis=1, keepdims=True)
            mixed = jnp.dot(weights.astype(BF16), kvr[1, g], preferred_element_type=F32)
            mixed += jnp.dot(near.astype(BF16), own_values, preferred_element_type=F32)
            mixed = (mixed / total).astype(BF16)
            rows = pl.ds(pl.multiple_of(token_row(c, z, co) + a * span, span), span)
            for g5 in range(per_head):
                ab[c, rows, g5 * HD : (g5 + 1) * HD] = mixed[g5 * span : (g5 + 1) * span, :]

    def project(c):
        total = jnp.zeros((feats, chunk_rows), F32)
        for k in range(heads):
            total += dot_last(
                wv[:, k * width : (k + 1) * width], ab[c, pl.ds(k * chunk_rows, chunk_rows), :]
            )
        hb[c, pl.ds(pl.multiple_of(me * feats, 16), feats), :] = total.astype(BF16)

    features = hb.shape[1]
    strip = HD

    def normalize(c):
        def squares(i, total):
            x = hb[c, pl.ds(pl.multiple_of(i * strip, strip), strip), :].astype(F32)
            return total + jnp.sum(x * x, axis=0, keepdims=True)

        total = lax.fori_loop(0, features // strip, squares, jnp.zeros((1, chunk_rows), F32))
        run_f[...] = lax.rsqrt(total / features + EPSILON)

    def weigh(i):
        rows = pl.ds(pl.multiple_of(i * WEIGH, 16), WEIGH)
        lv[rows, :] = (lv[rows, :].astype(F32) * gain[...]).astype(BF16)

    def chunk_ids(c):
        rows = []
        for i in range(side):
            d = (c * side + i) * CORES
            rows.append(smg[d, 0:1, :] + smg[d + 1, 0:1, :])
        ids = jnp.concatenate(rows, axis=1).astype(jnp.int32) - me * vocab
        return jnp.where(ids < vocab, ids, -1)

    def tile(c, v):
        ids_row = chunk_ids(c)
        part = TILE // PIECES
        peak, mass, hit = run_m[...], run_s[...], run_p[...]
        for piece in range(PIECES):
            first_row = v * TILE + piece * part
            rows = pl.ds(pl.multiple_of(first_row, 16), part)
            logits = jnp.dot(lv[rows, :], hb[c], preferred_element_type=F32) * run_f[...]
            at = lax.broadcasted_iota(jnp.int32, logits.shape, 0) + first_row
            logits = jnp.where(at < vocab, logits, NEGATIVE)
            hit += jnp.sum(jnp.where(at == ids_row, logits, 0.0), axis=0, keepdims=True)
            new = jnp.maximum(peak, jnp.max(logits, axis=0, keepdims=True))
            mass = mass * jnp.exp(peak - new) + jnp.sum(
                jnp.exp(logits - new), axis=0, keepdims=True
            )
            peak = new
        run_m[...] = peak
        run_s[...] = mass
        run_p[...] = hit

    def stats_send(c, i, core):
        d = (c * side + i) * CORES + core
        return d, send(st.at[c, i], sr.at[me], st_ss.at[d], st_rs.at[me], d)

    def stats_out(c):
        lse = run_m[...] + jnp.log(run_s[...])
        hit = run_p[...]
        for i in range(side):
            lanes = slice(i * HD, (i + 1) * HD)
            st[c, i, 0:1, :] = lse[:, lanes]
            st[c, i, 1:2, :] = hit[:, lanes]

        @pl.when(k0 == c)
        def _():
            own_lse, own_hit = lse[:, 0:HD], hit[:, 0:HD]
            for i in range(1, side):
                lanes = slice(i * HD, (i + 1) * HD)
                own_lse = jnp.where(j == i, lse[:, lanes], own_lse)
                own_hit = jnp.where(j == i, hit[:, lanes], own_hit)
            sr[me, 0:1, :] = own_lse
            sr[me, 1:2, :] = own_hit

        for i in range(side):
            for core in range(CORES):
                d, copy = stats_send(c, i, core)

                @pl.when(d != me)
                def _(copy=copy):
                    copy.start()

    tiles = -(-vocab // TILE)
    steps = []
    finished = 0
    while finished < tiles * CHUNKS:
        at = len(steps)
        steps.append(finished)
        ready = sum(at >= 2 * HALF + start for start in STARTS) * tiles
        finished = min(finished + PER_SLOT, ready)
    slots = len(steps)
    steps.append(finished)

    def slot(i, carry):
        for stream in range(CHUNKS):
            t = i - STARTS[stream]

            @pl.when(jnp.logical_and(t >= 1, t <= HALF))
            def _(stream=stream, t=t):
                with jax.named_scope(f"att{stream}"):
                    ring_step(stream, t)

        for stream in range(CHUNKS, 2 * CHUNKS):
            t = i - (STARTS[stream - CHUNKS] + HALF)

            @pl.when(jnp.logical_and(t >= 1, t <= HALF))
            def _(stream=stream, t=t):
                with jax.named_scope(f"hid{stream}"):
                    ring_step(stream, t)

        def begin(c, carry):
            with jax.named_scope("attention"):
                attention(c)
            attended_open(c)
            return carry

        begun = sum((i > start).astype(jnp.int32) for start in STARTS)
        due = sum((i >= start).astype(jnp.int32) for start in STARTS)
        lax.fori_loop(begun, due, begin, 0)

        @pl.when(i == HALF)
        def _():
            load_w.wait()

        @pl.when(i == 0)
        def _():
            load_lm.wait()

        @pl.when(i < lv.shape[0] // WEIGH)
        def _():
            with jax.named_scope("weigh"):
                weigh(i)

        for c in range(CHUNKS):

            @pl.when(i == STARTS[c] + HALF)
            def _(c=c):
                with jax.named_scope("partner1"):
                    ring_partner(c)
                with jax.named_scope("project"):
                    project(c)
                ring_open(CHUNKS + c)

        m = i - 2 * HALF

        @pl.when(m == 0)
        def _():
            def small_in(d, carry):
                @pl.when(d != me)
                def _():
                    send(smg.at[d], smg.at[d], sm_ss.at[d], sm_rs.at[d], partner).wait_recv()

                return carry

            lax.fori_loop(0, n, small_in, 0)

        for c in range(CHUNKS):

            @pl.when(m == STARTS[c])
            def _(c=c):
                with jax.named_scope("partner2"):
                    ring_partner(CHUNKS + c)

        first = 0
        last = 0
        for at in range(2 * HALF, slots):
            first = first + jnp.where(i > at, steps[at + 1] - steps[at], 0)
            last = last + jnp.where(i >= at, steps[at + 1] - steps[at], 0)

        def one(step, carry):
            c = lax.div(step, tiles)
            v = lax.rem(step, tiles)

            @pl.when(v == 0)
            def _():
                with jax.named_scope("norm"):
                    normalize(c)
                run_m[...] = jnp.full_like(run_m, NEGATIVE)
                run_s[...] = jnp.zeros_like(run_s)
                run_p[...] = jnp.zeros_like(run_p)

            with jax.named_scope("tile"):
                tile(c, v)

            @pl.when(v == tiles - 1)
            def _():
                with jax.named_scope("stats"):
                    stats_out(c)

            return carry

        lax.fori_loop(first, last, one, 0)
        return carry

    with jax.named_scope("slots"):
        lax.fori_loop(0, slots, slot, 0)

    every_reward = jnp.sum(smg[...][:, 1, :], axis=0, keepdims=True)[:, 0 : n * conts]
    advantages = []
    for a in range(conts):
        same = groups[...] == group_of[me * conts + a]
        mean = jnp.sum(jnp.where(same, every_reward, 0.0), axis=1, keepdims=True) / GROUP
        off = every_reward - mean
        spread = jnp.sum(jnp.where(same, off * off, 0.0), axis=1, keepdims=True)
        spread = jnp.sqrt(spread / (GROUP - 1))
        advantages.append((rewards[a] - mean) / jnp.maximum(spread, REWARD_FLOOR))

    def stats_in(d, carry):
        @pl.when(d != me)
        def _():
            send(sr.at[d], sr.at[d], st_ss.at[d], st_rs.at[d], partner).wait_recv()

        return carry

    with jax.named_scope("join"):
        lax.fori_loop(0, n, stats_in, 0)
    everyone = sr[...]
    lse = everyone[:, 0, :]
    peak = jnp.max(lse, axis=0, keepdims=True)
    lse = peak + jnp.log(jnp.sum(jnp.exp(lse - peak), axis=0, keepdims=True))
    logprob = jnp.sum(everyone[:, 1, :], axis=0, keepdims=True) - lse
    logprob = jnp.where(co == 0, logprob[:, 0:own], logprob[:, own : 2 * own])
    position = lax.broadcasted_iota(jnp.int32, (1, span), 1)
    for a in range(conts):
        live = jnp.where(position < cont_len[a], logprob[:, a * span : (a + 1) * span], 0.0)
        out_logprob[a : a + 1, :] = live
        gained = advantages[a] * jnp.sum(live, axis=1, keepdims=True)
        gained = gained / jnp.full((1, 1), cont_len[a], jnp.int32).astype(F32)
        out_advantage[a] = advantages[a][0, 0]
        out_objective[a] = gained[0, 0]

    @pl.when(j >= side // 2)
    def _():
        far_right.wait_send()

    @pl.when(j < side // 2)
    def _():
        far_left.wait_send()

    ext_right.wait_send()
    ext_left.wait_send()

    @pl.when(j < side - 1)
    def _():
        own_right.wait_send()

    @pl.when(j > 0)
    def _():
        own_left.wait_send()

    own_part.wait_send()
    for step in range(1, heads):
        q_send(step).wait_send()

    def chain_out(i, carry):
        t = i + 1

        @pl.when(t <= j + reach)
        def _():
            @pl.when(j < side - 1)
            def _():
                up_send(t).wait_send()

            kv_d2d(z - t, kv_at(z - t)).wait_send()

        @pl.when(t <= side - 1 - j + reach)
        def _():
            @pl.when(j > 0)
            def _():
                down_send(t).wait_send()

            kv_d2d(z + t, kv_at(z + t)).wait_send()

        return carry

    lax.fori_loop(0, longest, chain_out, 0)

    def peers_out(d, carry):
        @pl.when(d != me)
        def _():
            small_send(d).wait_send()
            send(st.at[0, 0], sr.at[me], st_ss.at[d], st_rs.at[me], d).wait_send()

        return carry

    lax.fori_loop(0, n, peers_out, 0)

    def ring_out(t, carry):
        for stream in range(2 * CHUNKS):
            right, left = steps_of(stream)

            @pl.when(t < right)
            def _(stream=stream):
                ring_right(stream, t).wait_send()

            @pl.when(t < left)
            def _(stream=stream):
                ring_left(stream, t).wait_send()

            ring_d2d(stream, t).wait_send()
            ring_d2d(stream, t + HALF).wait_send()
        return carry

    lax.fori_loop(0, HALF, ring_out, 0)


def scores_of(
    n, group_of, prompt_len, rewards, cont_len, groups, ids, gain, q, ck, cv, pk, pv, wt, lm
):
    conts, span, query_width = q.shape
    prompts, positions, kv_width = pk.shape
    heads = kv_width // HD
    per_head = query_width // kv_width
    chips = n // CORES
    own = conts * span
    feats, features = wt.shape
    vocab = lm.shape[0]
    chunk_rows = n // CHUNKS * own
    chunk_q = own * per_head + 2 * own
    streams = 2 * CHUNKS
    side = chips // heads
    dims = (n, heads, per_head, conts, span, positions)
    dma = pltpu.SemaphoreType.DMA
    vmem_rows = -(-vocab // TILE) * TILE
    any_spec = pl.BlockSpec(memory_space=pl.ANY)
    smem_spec = pl.BlockSpec(memory_space=pltpu.SMEM)
    vmem_spec = pl.BlockSpec(memory_space=pltpu.VMEM)
    return pl.pallas_call(
        functools.partial(kernel, dims),
        out_shape=(
            jax.ShapeDtypeStruct((conts, span), F32),
            jax.ShapeDtypeStruct((conts,), F32),
            jax.ShapeDtypeStruct((conts,), F32),
        ),
        in_specs=[smem_spec] * 4 + [vmem_spec] * 3 + [any_spec] * 7,
        out_specs=(vmem_spec, smem_spec, smem_spec),
        scratch_shapes=[
            pltpu.VMEM((heads, 2, prompts, positions, HD), BF16),
            pltpu.VMEM((2, prompts, n * positions, HD), BF16),
            pltpu.VMEM((heads, chunk_q, HD), BF16),
            pltpu.VMEM((heads, chunk_q, HD), BF16),
            pltpu.VMEM((CHUNKS, n * own, per_head * HD), BF16),
            pltpu.VMEM((CHUNKS, n * feats, chunk_rows), BF16),
            pltpu.VMEM((feats, features), BF16),
            pltpu.VMEM((vmem_rows, n * feats), BF16),
            pltpu.VMEM((2, HD), F32),
            pltpu.VMEM((n, 2, HD), F32),
            pltpu.VMEM((1, chunk_rows), F32),
            pltpu.VMEM((1, chunk_rows), F32),
            pltpu.VMEM((1, chunk_rows), F32),
            pltpu.VMEM((1, chunk_rows), F32),
            pltpu.VMEM((CHUNKS, side, 2, HD), F32),
            pltpu.VMEM((n, 2, HD), F32),
            dma((9,)),
            dma((chips,)),
            dma((chips,)),
            dma((6,)),
            dma((chips,)),
            dma((chips,)),
            dma((chips,)),
            dma((heads,)),
            dma((heads,)),
            dma((n,)),
            dma((n,)),
            dma((streams, chips)),
            dma((streams, chips)),
            dma((streams, HALF)),
            dma((streams, HALF)),
            dma((streams, chips)),
            dma((n,)),
            dma((n,)),
        ],
        compiler_params=pltpu.CompilerParams(
            collective_id=0, has_side_effects=True, vmem_limit_bytes=67_043_328
        ),
        name="scores",
    )(group_of, prompt_len, rewards, cont_len, groups, ids, gain, q, ck, cv, pk, pv, wt, lm)


def per_device(
    n,
    cont_query,
    cont_key,
    cont_value,
    prefix_key,
    prefix_value,
    out_weight,
    norm_gain,
    lm_head,
    target_ids,
    cont_len,
    prompt_len,
    group_of,
    rewards,
):
    return scores_of(
        n,
        group_of,
        prompt_len,
        rewards,
        cont_len,
        group_of.reshape(1, -1),
        target_ids,
        norm_gain.reshape(1, -1),
        cont_query,
        cont_key,
        cont_value,
        prefix_key,
        prefix_value,
        out_weight.T,
        lm_head.T,
    )


def solution(mesh):
    both = ("grp", "seq")
    in_specs = (
        P(both, None, None),
        P(both, None, None),
        P(both, None, None),
        P("grp", "seq", None),
        P("grp", "seq", None),
        P(None, "seq"),
        P(),
        P(None, "seq"),
        P(both, None),
        P(both),
        P("grp"),
        P("grp"),
        P(both),
    )
    out_specs = (P(both, None), P(both), P(both))
    return jax.shard_map(
        functools.partial(per_device, mesh.shape["seq"]),
        mesh=mesh,
        in_specs=in_specs,
        out_specs=out_specs,
        check_vma=False,
    )
```

```python
import functools

import jax
import jax.numpy as jnp
from jax import lax
from jax.experimental import pallas as pl
from jax.experimental.pallas import tpu as pltpu
from jax.sharding import PartitionSpec as P

HD = 128
GROUP = 16
NEGATIVE = -1e30
EPSILON = 1e-06
REWARD_FLOOR = 0.25

Q_AT = (0, 3, 5, 3)
CORES = 2
CHUNKS = 4
STARTS = (0, 0, 5, 7)
PER_SLOT = 2
TILE = 480
PIECES = 3
WEIGH = 160
HALF = 8

BF16 = jnp.bfloat16
F32 = jnp.float32


def dot_last(a, b):
    return lax.dot_general(a, b, (((1,), (1,)), ((), ())), preferred_element_type=F32)


def send(src, dst, send_sem, recv_sem, device):
    return pltpu.make_async_remote_copy(
        src_ref=src,
        dst_ref=dst,
        send_sem=send_sem,
        recv_sem=recv_sem,
        device_id={"seq": device},
        device_id_type=pl.DeviceIdType.MESH,
    )


def kernel(
    dims,
    group_of,
    prompt_len,
    rewards,
    cont_len,
    groups,
    ids,
    gain,
    q,
    ck,
    cv,
    pk,
    pv,
    wt,
    lm,
    out,
    kvs,
    kvr,
    qs,
    qr,
    ab,
    hb,
    wv,
    gv,
    lv,
    smv,
    smg,
    run_f,
    run_m,
    run_s,
    run_p,
    st,
    sr,
    loc,
    kv_rs,
    kv_rd,
    kv_so,
    kv_sd,
    kv_su,
    kv_sn,
    q_rs,
    q_ss,
    sm_rs,
    sm_ss,
    g_rs,
    g_rd,
    g_sr,
    g_sl,
    g_sd,
    st_rs,
    st_ss,
):
    n, heads, per_head, conts, span, positions = dims
    chips = n // CORES
    side = chips // heads
    vocab = lm.shape[0]
    rows_q = conts * per_head * span
    one_q = per_head * span
    own = conts * span
    feats = wt.shape[0]
    width = per_head * HD
    chunk_rows = n // CHUNKS * own

    me = lax.axis_index("seq")
    z = lax.div(me, CORES)
    co = lax.rem(me, CORES)
    partner = me + 1 - 2 * co
    k0 = lax.div(z, side)
    j = lax.rem(z, side)
    base = k0 * side

    def chip(at):
        return lax.rem(at + chips, chips)

    def dev(at):
        return chip(at) * CORES + co

    barrier = pltpu.get_barrier_semaphore()

    def greet(d, carry):
        @pl.when(d != me)
        def _():
            pl.semaphore_signal(
                barrier, inc=1, device_id={"seq": d}, device_id_type=pl.DeviceIdType.MESH
            )

        return carry

    lax.fori_loop(0, n, greet, 0)

    def kv_loads(head):
        lanes = pl.ds(pl.multiple_of(head * HD, HD), HD)
        return lanes

    def load_kv(head, carry):
        lanes = kv_loads(head)
        pltpu.make_async_copy(pk.at[:, :, lanes], kvs.at[head, 0], loc.at[0]).start()
        pltpu.make_async_copy(pv.at[:, :, lanes], kvs.at[head, 1], loc.at[0]).start()
        return carry

    lax.fori_loop(0, heads, load_kv, 0)

    def load_q(head, carry):
        for a in range(conts):
            for g in range(per_head):
                lanes = pl.ds(pl.multiple_of((head * per_head + g) * HD, HD), HD)
                pltpu.make_async_copy(
                    q.at[a, :, lanes], qs.at[head, pl.ds(a * one_q + g * span, span), :], loc.at[1]
                ).start()
            lanes = pl.ds(pl.multiple_of(head * HD, HD), HD)
            pltpu.make_async_copy(
                ck.at[a, :, lanes], qs.at[head, pl.ds(rows_q + a * span, span), :], loc.at[1]
            ).start()
            pltpu.make_async_copy(
                cv.at[a, :, lanes], qs.at[head, pl.ds(rows_q + own + a * span, span), :], loc.at[1]
            ).start()
        return carry

    lax.fori_loop(0, heads, load_q, 0)

    lane = lax.broadcasted_iota(jnp.int32, (1, HD), 1)
    own_ids = ids[...].astype(F32)
    own_ids = jnp.concatenate([own_ids[a : a + 1, :] for a in range(conts)] * CORES, axis=1)
    own_ids = jnp.where(lax.div(lane, own) == co, own_ids, 0.0)
    own_rewards = jnp.zeros((1, HD), F32)
    for a in range(conts):
        own_rewards = jnp.where(lane == me * conts + a, rewards[a], own_rewards)
    smv[0:1, :] = own_ids
    smv[1:2, :] = own_rewards
    smg[me, 0:1, :] = own_ids
    smg[me, 1:2, :] = own_rewards

    with jax.named_scope("greet"):
        pltpu.make_async_copy(kvs, kvs, loc.at[0]).wait()
        pl.semaphore_wait(barrier, n - 1)

    def kv_at(src):
        rows = pl.ds(pl.multiple_of((chip(src) * CORES + co) * positions, positions), positions)
        return kvr.at[:, :, rows, :]

    def kv_sem(src):
        return chip(src)

    def kv_send(source, head_block, target, send_sem):
        return send(head_block, kv_at(source), send_sem, kv_rs.at[kv_sem(source)], dev(target))

    def kv_d2d(source, block):
        return send(
            block, kv_at(source), kv_sd.at[kv_sem(source)], kv_rd.at[kv_sem(source)], partner
        )

    next_head = lax.rem(k0 + 1, heads)
    prev_head = lax.rem(k0 + heads - 1, heads)
    far_head = lax.rem(k0 + 2, heads)
    own_right = kv_send(z, kvs.at[k0], z + 1, kv_so.at[0])
    own_left = kv_send(z, kvs.at[k0], z - 1, kv_so.at[1])
    ext_right = kv_send(z, kvs.at[next_head], base + side, kv_so.at[2])
    ext_left = kv_send(z, kvs.at[prev_head], base - 1, kv_so.at[3])
    far_right = kv_send(z, kvs.at[far_head], base + 2 * side, kv_so.at[4])
    far_left = kv_send(z, kvs.at[far_head], base - side - 1, kv_so.at[5])
    own_part = kv_d2d(z, kvs.at[k0])

    @pl.when(j < side - 1)
    def _():
        own_right.start()

    @pl.when(j > 0)
    def _():
        own_left.start()

    own_part.start()
    own_rows = pl.ds(pl.multiple_of(me * positions, positions), positions)
    own_lanes = pl.ds(pl.multiple_of(k0 * HD, HD), HD)
    keep_k = pltpu.make_async_copy(pk.at[:, :, own_lanes], kvr.at[0, :, own_rows, :], loc.at[3])
    keep_v = pltpu.make_async_copy(pv.at[:, :, own_lanes], kvr.at[1, :, own_rows, :], loc.at[4])
    keep_k.start()
    keep_v.start()

    pltpu.make_async_copy(qs, qs, loc.at[1]).wait()

    def q_send(step):
        target = chip(z + side * step)
        if 2 * step == heads:
            shifted = jnp.where(j >= side // 2, side * step - side // 2, side * step + side // 2)
            target = chip(z + shifted)
        return send(
            qs.at[lax.div(target, side)],
            qr.at[k0],
            q_ss.at[step],
            q_rs.at[k0],
            dev(target),
        )

    keep_q = []
    for a in range(conts):
        for g in range(per_head):
            lanes = pl.ds(pl.multiple_of((k0 * per_head + g) * HD, HD), HD)
            keep_q.append((q.at[a, :, lanes], pl.ds(a * one_q + g * span, span)))
        keep_q.append((ck.at[a, :, own_lanes], pl.ds(rows_q + a * span, span)))
        keep_q.append((cv.at[a, :, own_lanes], pl.ds(rows_q + own + a * span, span)))
    for source, rows in keep_q:
        pltpu.make_async_copy(source, qr.at[k0, rows, :], loc.at[5]).start()


    def small_send(d):
        return send(smv, smg.at[me], sm_ss.at[d], sm_rs.at[me], d)

    def small_out(d, carry):
        @pl.when(d != me)
        def _():
            small_send(d).start()

        return carry

    with jax.named_scope("small"):
        lax.fori_loop(0, n, small_out, 0)
    load_w = pltpu.make_async_copy(wt, wv, loc.at[6])
    load_w.start()
    load_lm = pltpu.make_async_copy(lm, lv.at[pl.ds(0, vocab), :], loc.at[2])
    load_lm.start()

    reach = side + side // 2

    def up_send(t):
        return kv_send(z - t, kv_at(z - t), z + 1, kv_su.at[t - 1])

    def down_send(t):
        return kv_send(z + t, kv_at(z + t), z - 1, kv_sn.at[t - 1])

    def depart(i):
        @pl.when(i == side - 1 - j)
        def _():
            ext_right.start()

        @pl.when(i == j)
        def _():
            ext_left.start()

        @pl.when(jnp.logical_and(j >= side // 2, i == 2 * (side - 1) - j))
        def _():
            far_right.start()

        @pl.when(jnp.logical_and(j < side // 2, i == side - 1 + j))
        def _():
            far_left.start()

        for step in range(1, heads):

            @pl.when(i == Q_AT[step])
            def _(step=step):
                q_send(step).start()

    def chain(i, carry):
        t = i + 1
        depart(i)

        @pl.when(t <= j + reach)
        def _():
            kv_send(z - t, kv_at(z - t), z + 1, kv_su.at[t - 1]).wait_recv()

            @pl.when(j < side - 1)
            def _():
                up_send(t).start()

            kv_d2d(z - t, kv_at(z - t)).start()

        @pl.when(t <= side - 1 - j + reach)
        def _():
            kv_send(z + t, kv_at(z + t), z - 1, kv_sn.at[t - 1]).wait_recv()

            @pl.when(j > 0)
            def _():
                down_send(t).start()

            kv_d2d(z + t, kv_at(z + t)).start()

        return carry

    longest = side - 1 + reach
    with jax.named_scope("chain"):
        lax.fori_loop(0, longest, chain, 0)

    keep_k.wait()
    keep_v.wait()
    pltpu.make_async_copy(qr.at[k0], qr.at[k0], loc.at[5]).wait()

    def other_rows(src):
        rows = pl.ds(
            pl.multiple_of((src * CORES + 1 - co) * positions, positions), positions
        )
        return kvr.at[:, :, rows, :]

    def kv_partner(src, carry):
        send(other_rows(src), other_rows(src), kv_sd.at[src], kv_rd.at[src], partner).wait_recv()
        return carry

    with jax.named_scope("kvpartner"):
        lax.fori_loop(0, chips, kv_partner, 0)

    def q_arrived(c, carry):
        @pl.when(c != k0)
        def _():
            send(qr.at[c], qr.at[c], q_ss.at[0], q_rs.at[c], partner).wait_recv()

        return carry

    with jax.named_scope("qarrive"):
        lax.fori_loop(0, heads, q_arrived, 0)

    def place_of(c, chip_id):
        k = lax.div(chip_id, side)
        away = lax.rem(c - k + heads, heads)
        place = lax.rem(chip_id, side)
        return jnp.where(2 * away == heads, lax.rem(place + side // 2, side), place)

    def token_row(c, chip_id, core):
        k = lax.div(chip_id, side)
        return ((k * side + place_of(c, chip_id)) * CORES + core) * own

    def block_at(stream, chip_id, core):
        d = chip(chip_id) * CORES + core
        if stream < CHUNKS:
            at = token_row(stream, chip(chip_id), core)
            return ab.at[stream, pl.ds(pl.multiple_of(at, own), own), :]
        return hb.at[stream - CHUNKS, pl.ds(pl.multiple_of(d * feats, 16), feats), :]

    def ring_send(stream, source, target, send_sem):
        block = block_at(stream, source, co)
        return send(block, block, send_sem, g_rs.at[stream, chip(source)], dev(target))

    def ring_right(stream, t):
        return ring_send(stream, z - t, z + 1, g_sr.at[stream, t])

    def ring_left(stream, t):
        return ring_send(stream, z + t, z - 1, g_sl.at[stream, t])

    def ring_d2d(stream, source):
        block = block_at(stream, source, co)
        return send(
            block, block, g_sd.at[stream, chip(source)], g_rd.at[stream, chip(source)], partner
        )

    def steps_of(stream):
        right = HALF if stream % 2 == 0 else chips - 1 - HALF
        return right, chips - 1 - right

    def ring_open(stream):
        ring_right(stream, 0).start()
        ring_left(stream, 0).start()
        ring_d2d(stream, z).start()

    def attended_open(c):
        rows = pl.ds(pl.multiple_of(token_row(c, z, co), own), own)
        block = ab.at[c, rows, :]
        send(block, block, g_sr.at[c, 0], g_rs.at[c, z], dev(z + 1)).start()
        send(block, block, g_sl.at[c, 0], g_rs.at[c, z], dev(z - 1)).start()
        send(block, block, g_sd.at[c, z], g_rd.at[c, z], partner).start()

    def ring_step(stream, t):
        right, left = steps_of(stream)

        @pl.when(t <= right)
        def _():
            ring_send(stream, z - t, z + 1, g_sr.at[stream, 0]).wait_recv()

            @pl.when(t < right)
            def _():
                ring_right(stream, t).start()

        @pl.when(t <= left)
        def _():
            ring_send(stream, z + t, z - 1, g_sl.at[stream, 0]).wait_recv()

            @pl.when(t < left)
            def _():
                ring_left(stream, t).start()

        @pl.when(t <= right)
        def _():
            ring_d2d(stream, z - t).start()

        @pl.when(t <= left)
        def _():
            ring_d2d(stream, z + t).start()

    def ring_partner(stream):
        def arrived(src, carry):
            block = block_at(stream, src, 1 - co)
            send(
                block, block, g_sd.at[stream, src], g_rd.at[stream, src], partner
            ).wait_recv()
            return carry

        lax.fori_loop(0, chips, arrived, 0)

    def attention(c):
        for a in range(conts):
            cont = ((c * side + place_of(c, z)) * CORES + co) * conts + a
            g = group_of[cont]
            length = prompt_len[g]
            queries = qr[c, pl.ds(a * one_q, one_q), :]
            own_keys = qr[c, pl.ds(rows_q + a * span, span), :]
            own_values = qr[c, pl.ds(rows_q + own + a * span, span), :]
            scores = dot_last(queries, kvr[0, g]) * HD ** (-0.5)
            at = lax.broadcasted_iota(jnp.int32, scores.shape, 1)
            scores = jnp.where(at < length, scores, NEGATIVE)
            near = dot_last(queries, own_keys) * HD ** (-0.5)
            token = lax.rem(lax.broadcasted_iota(jnp.int32, near.shape, 0), span)
            near = jnp.where(lax.broadcasted_iota(jnp.int32, near.shape, 1) <= token, near, NEGATIVE)
            peak = jnp.maximum(
                jnp.max(scores, axis=1, keepdims=True), jnp.max(near, axis=1, keepdims=True)
            )
            weights = jnp.exp(scores - peak)
            near = jnp.exp(near - peak)
            total = jnp.sum(weights, axis=1, keepdims=True) + jnp.sum(near, axis=1, keepdims=True)
            mixed = jnp.dot(weights.astype(BF16), kvr[1, g], preferred_element_type=F32)
            mixed += jnp.dot(near.astype(BF16), own_values, preferred_element_type=F32)
            mixed = (mixed / total).astype(BF16)
            rows = pl.ds(pl.multiple_of(token_row(c, z, co) + a * span, span), span)
            for g5 in range(per_head):
                ab[c, rows, g5 * HD : (g5 + 1) * HD] = mixed[g5 * span : (g5 + 1) * span, :]

    def project(c):
        total = jnp.zeros((feats, chunk_rows), F32)
        for k in range(heads):
            total += dot_last(
                wv[:, k * width : (k + 1) * width], ab[c, pl.ds(k * chunk_rows, chunk_rows), :]
            )
        hb[c, pl.ds(pl.multiple_of(me * feats, 16), feats), :] = total.astype(BF16)

    features = hb.shape[1]
    strip = HD

    def normalize(c):
        def squares(i, total):
            x = hb[c, pl.ds(pl.multiple_of(i * strip, strip), strip), :].astype(F32)
            return total + jnp.sum(x * x, axis=0, keepdims=True)

        total = lax.fori_loop(0, features // strip, squares, jnp.zeros((1, chunk_rows), F32))
        run_f[...] = lax.rsqrt(total / features + EPSILON)

    def weigh(i):
        rows = pl.ds(pl.multiple_of(i * WEIGH, 16), WEIGH)
        lv[rows, :] = (lv[rows, :].astype(F32) * gv[...]).astype(BF16)

    def chunk_ids(c):
        rows = []
        for i in range(side):
            d = (c * side + i) * CORES
            rows.append(smg[d, 0:1, :] + smg[d + 1, 0:1, :])
        ids = jnp.concatenate(rows, axis=1).astype(jnp.int32) - me * vocab
        return jnp.where(ids < vocab, ids, -1)

    def tile(c, v):
        ids_row = chunk_ids(c)
        part = TILE // PIECES
        peak, mass, hit = run_m[...], run_s[...], run_p[...]
        for piece in range(PIECES):
            first_row = v * TILE + piece * part
            rows = pl.ds(pl.multiple_of(first_row, 16), part)
            logits = jnp.dot(lv[rows, :], hb[c], preferred_element_type=F32) * run_f[...]
            at = lax.broadcasted_iota(jnp.int32, logits.shape, 0) + first_row
            logits = jnp.where(at < vocab, logits, NEGATIVE)
            hit += jnp.sum(jnp.where(at == ids_row, logits, 0.0), axis=0, keepdims=True)
            new = jnp.maximum(peak, jnp.max(logits, axis=0, keepdims=True))
            mass = mass * jnp.exp(peak - new) + jnp.sum(
                jnp.exp(logits - new), axis=0, keepdims=True
            )
            peak = new
        run_m[...] = peak
        run_s[...] = mass
        run_p[...] = hit

    def stats_send(c, i, core):
        d = (c * side + i) * CORES + core
        return d, send(st.at[c, i], sr.at[me], st_ss.at[d], st_rs.at[me], d)

    def stats_out(c):
        lse = run_m[...] + jnp.log(run_s[...])
        hit = run_p[...]
        for i in range(side):
            lanes = slice(i * HD, (i + 1) * HD)
            st[c, i, 0:1, :] = lse[:, lanes]
            st[c, i, 1:2, :] = hit[:, lanes]

        @pl.when(k0 == c)
        def _():
            own_lse, own_hit = lse[:, 0:HD], hit[:, 0:HD]
            for i in range(1, side):
                lanes = slice(i * HD, (i + 1) * HD)
                own_lse = jnp.where(j == i, lse[:, lanes], own_lse)
                own_hit = jnp.where(j == i, hit[:, lanes], own_hit)
            sr[me, 0:1, :] = own_lse
            sr[me, 1:2, :] = own_hit

        for i in range(side):
            for core in range(CORES):
                d, copy = stats_send(c, i, core)

                @pl.when(d != me)
                def _(copy=copy):
                    copy.start()

    tiles = -(-vocab // TILE)
    steps = []
    finished = 0
    while finished < tiles * CHUNKS:
        at = len(steps)
        steps.append(finished)
        ready = sum(at >= 2 * HALF + start for start in STARTS) * tiles
        finished = min(finished + PER_SLOT, ready)
    slots = len(steps)
    steps.append(finished)

    def slot(i, carry):
        for stream in range(CHUNKS):
            t = i - STARTS[stream]

            @pl.when(jnp.logical_and(t >= 1, t <= HALF))
            def _(stream=stream, t=t):
                with jax.named_scope(f"att{stream}"):
                    ring_step(stream, t)

        for stream in range(CHUNKS, 2 * CHUNKS):
            t = i - (STARTS[stream - CHUNKS] + HALF)

            @pl.when(jnp.logical_and(t >= 1, t <= HALF))
            def _(stream=stream, t=t):
                with jax.named_scope(f"hid{stream}"):
                    ring_step(stream, t)

        def begin(c, carry):
            with jax.named_scope("attention"):
                attention(c)
            attended_open(c)
            return carry

        begun = sum((i > start).astype(jnp.int32) for start in STARTS)
        due = sum((i >= start).astype(jnp.int32) for start in STARTS)
        lax.fori_loop(begun, due, begin, 0)

        @pl.when(i == HALF)
        def _():
            load_w.wait()

        @pl.when(i == 0)
        def _():
            load_lm.wait()
            for row in range(gain.shape[0]):
                gv[0:1, row * HD : (row + 1) * HD] = gain[row : row + 1, :]

        @pl.when(i < lv.shape[0] // WEIGH)
        def _():
            with jax.named_scope("weigh"):
                weigh(i)

        for c in range(CHUNKS):

            @pl.when(i == STARTS[c] + HALF)
            def _(c=c):
                with jax.named_scope("partner1"):
                    ring_partner(c)
                with jax.named_scope("project"):
                    project(c)
                ring_open(CHUNKS + c)

        m = i - 2 * HALF

        @pl.when(m == 0)
        def _():
            def small_in(d, carry):
                @pl.when(d != me)
                def _():
                    send(smg.at[d], smg.at[d], sm_ss.at[d], sm_rs.at[d], partner).wait_recv()

                return carry

            lax.fori_loop(0, n, small_in, 0)

        for c in range(CHUNKS):

            @pl.when(m == STARTS[c])
            def _(c=c):
                with jax.named_scope("partner2"):
                    ring_partner(CHUNKS + c)

        first = 0
        last = 0
        for at in range(2 * HALF, slots):
            first = first + jnp.where(i > at, steps[at + 1] - steps[at], 0)
            last = last + jnp.where(i >= at, steps[at + 1] - steps[at], 0)

        def one(step, carry):
            c = lax.div(step, tiles)
            v = lax.rem(step, tiles)

            @pl.when(v == 0)
            def _():
                with jax.named_scope("norm"):
                    normalize(c)
                run_m[...] = jnp.full_like(run_m, NEGATIVE)
                run_s[...] = jnp.zeros_like(run_s)
                run_p[...] = jnp.zeros_like(run_p)

            with jax.named_scope("tile"):
                tile(c, v)

            @pl.when(v == tiles - 1)
            def _():
                with jax.named_scope("stats"):
                    stats_out(c)

            return carry

        lax.fori_loop(first, last, one, 0)
        return carry

    with jax.named_scope("slots"):
        lax.fori_loop(0, slots, slot, 0)

    every_reward = jnp.sum(smg[...][:, 1, :], axis=0, keepdims=True)[:, 0 : n * conts]
    advantages = []
    for a in range(conts):
        same = groups[...] == group_of[me * conts + a]
        mean = jnp.sum(jnp.where(same, every_reward, 0.0), axis=1, keepdims=True) / GROUP
        off = every_reward - mean
        spread = jnp.sum(jnp.where(same, off * off, 0.0), axis=1, keepdims=True)
        spread = jnp.sqrt(spread / (GROUP - 1))
        advantages.append((rewards[a] - mean) / jnp.maximum(spread, REWARD_FLOOR))

    def stats_in(d, carry):
        @pl.when(d != me)
        def _():
            send(sr.at[d], sr.at[d], st_ss.at[d], st_rs.at[d], partner).wait_recv()

        return carry

    with jax.named_scope("join"):
        lax.fori_loop(0, n, stats_in, 0)
    everyone = sr[...]
    lse = everyone[:, 0, :]
    peak = jnp.max(lse, axis=0, keepdims=True)
    lse = peak + jnp.log(jnp.sum(jnp.exp(lse - peak), axis=0, keepdims=True))
    logprob = jnp.sum(everyone[:, 1, :], axis=0, keepdims=True) - lse
    logprob = jnp.where(co == 0, logprob[:, 0:own], logprob[:, own : 2 * own])
    position = lax.broadcasted_iota(jnp.int32, (1, span), 1)
    gains = jnp.zeros((1, HD), F32)
    objectives = jnp.zeros((1, HD), F32)
    for a in range(conts):
        live = jnp.where(position < cont_len[a], logprob[:, a * span : (a + 1) * span], 0.0)
        out[a : a + 1, 0:span] = live
        gained = advantages[a] * jnp.sum(live, axis=1, keepdims=True)
        gained = gained / jnp.full((1, 1), cont_len[a], jnp.int32).astype(F32)
        gains = jnp.where(lane == a, advantages[a], gains)
        objectives = jnp.where(lane == a, gained, objectives)
    out[conts : conts + 1, :] = gains
    out[conts + 1 : conts + 2, :] = objectives

    @pl.when(j >= side // 2)
    def _():
        far_right.wait_send()

    @pl.when(j < side // 2)
    def _():
        far_left.wait_send()

    ext_right.wait_send()
    ext_left.wait_send()

    @pl.when(j < side - 1)
    def _():
        own_right.wait_send()

    @pl.when(j > 0)
    def _():
        own_left.wait_send()

    own_part.wait_send()
    for step in range(1, heads):
        q_send(step).wait_send()

    def chain_out(i, carry):
        t = i + 1

        @pl.when(t <= j + reach)
        def _():
            @pl.when(j < side - 1)
            def _():
                up_send(t).wait_send()

            kv_d2d(z - t, kv_at(z - t)).wait_send()

        @pl.when(t <= side - 1 - j + reach)
        def _():
            @pl.when(j > 0)
            def _():
                down_send(t).wait_send()

            kv_d2d(z + t, kv_at(z + t)).wait_send()

        return carry

    lax.fori_loop(0, longest, chain_out, 0)

    def peers_out(d, carry):
        @pl.when(d != me)
        def _():
            small_send(d).wait_send()
            send(st.at[0, 0], sr.at[me], st_ss.at[d], st_rs.at[me], d).wait_send()

        return carry

    lax.fori_loop(0, n, peers_out, 0)

    def ring_out(t, carry):
        for stream in range(2 * CHUNKS):
            right, left = steps_of(stream)

            @pl.when(t < right)
            def _(stream=stream):
                ring_right(stream, t).wait_send()

            @pl.when(t < left)
            def _(stream=stream):
                ring_left(stream, t).wait_send()

            ring_d2d(stream, t).wait_send()
            ring_d2d(stream, t + HALF).wait_send()
        return carry

    lax.fori_loop(0, HALF, ring_out, 0)


def scores_of(
    n, group_of, prompt_len, rewards, cont_len, groups, ids, gain, q, ck, cv, pk, pv, wt, lm
):
    conts, span, query_width = q.shape
    prompts, positions, kv_width = pk.shape
    heads = kv_width // HD
    per_head = query_width // kv_width
    chips = n // CORES
    own = conts * span
    feats, features = wt.shape
    vocab = lm.shape[0]
    chunk_rows = n // CHUNKS * own
    chunk_q = own * per_head + 2 * own
    streams = 2 * CHUNKS
    side = chips // heads
    dims = (n, heads, per_head, conts, span, positions)
    dma = pltpu.SemaphoreType.DMA
    vmem_rows = -(-vocab // TILE) * TILE
    any_spec = pl.BlockSpec(memory_space=pl.ANY)
    smem_spec = pl.BlockSpec(memory_space=pltpu.SMEM)
    vmem_spec = pl.BlockSpec(memory_space=pltpu.VMEM)
    return pl.pallas_call(
        functools.partial(kernel, dims),
        out_shape=jax.ShapeDtypeStruct((8, HD), F32),
        in_specs=[smem_spec] * 4 + [vmem_spec] * 3 + [any_spec] * 7,
        out_specs=vmem_spec,
        scratch_shapes=[
            pltpu.VMEM((heads, 2, prompts, positions, HD), BF16),
            pltpu.VMEM((2, prompts, n * positions, HD), BF16),
            pltpu.VMEM((heads, chunk_q, HD), BF16),
            pltpu.VMEM((heads, chunk_q, HD), BF16),
            pltpu.VMEM((CHUNKS, n * own, per_head * HD), BF16),
            pltpu.VMEM((CHUNKS, n * feats, chunk_rows), BF16),
            pltpu.VMEM((feats, features), BF16),
            pltpu.VMEM((1, n * feats), F32),
            pltpu.VMEM((vmem_rows, n * feats), BF16),
            pltpu.VMEM((2, HD), F32),
            pltpu.VMEM((n, 2, HD), F32),
            pltpu.VMEM((1, chunk_rows), F32),
            pltpu.VMEM((1, chunk_rows), F32),
            pltpu.VMEM((1, chunk_rows), F32),
            pltpu.VMEM((1, chunk_rows), F32),
            pltpu.VMEM((CHUNKS, side, 2, HD), F32),
            pltpu.VMEM((n, 2, HD), F32),
            dma((9,)),
            dma((chips,)),
            dma((chips,)),
            dma((6,)),
            dma((chips,)),
            dma((chips,)),
            dma((chips,)),
            dma((heads,)),
            dma((heads,)),
            dma((n,)),
            dma((n,)),
            dma((streams, chips)),
            dma((streams, chips)),
            dma((streams, HALF)),
            dma((streams, HALF)),
            dma((streams, chips)),
            dma((n,)),
            dma((n,)),
        ],
        compiler_params=pltpu.CompilerParams(
            collective_id=0, has_side_effects=True, vmem_limit_bytes=67_043_328
        ),
        name="scores",
    )(group_of, prompt_len, rewards, cont_len, groups, ids, gain, q, ck, cv, pk, pv, wt, lm)


def per_device(
    n,
    cont_query,
    cont_key,
    cont_value,
    prefix_key,
    prefix_value,
    out_weight,
    norm_gain,
    lm_head,
    target_ids,
    cont_len,
    prompt_len,
    group_of,
    rewards,
):
    found = scores_of(
        n,
        group_of,
        prompt_len,
        rewards,
        cont_len,
        group_of.reshape(1, -1),
        target_ids,
        norm_gain.reshape(-1, HD),
        cont_query,
        cont_key,
        cont_value,
        prefix_key,
        prefix_value,
        out_weight.T,
        lm_head.T,
    )
    conts, span, _ = cont_query.shape
    return (found[:conts, :span], found[conts, :conts], found[conts + 1, :conts])


def solution(mesh):
    both = ("grp", "seq")
    in_specs = (
        P(both, None, None),
        P(both, None, None),
        P(both, None, None),
        P("grp", "seq", None),
        P("grp", "seq", None),
        P(None, "seq"),
        P(),
        P(None, "seq"),
        P(both, None),
        P(both),
        P("grp"),
        P("grp"),
        P(both),
    )
    out_specs = (P(both, None), P(both), P(both))
    return jax.shard_map(
        functools.partial(per_device, mesh.shape["seq"]),
        mesh=mesh,
        in_specs=in_specs,
        out_specs=out_specs,
        check_vma=False,
    )
```

```python
import functools

import jax
import jax.numpy as jnp
from jax import lax
from jax.experimental import pallas as pl
from jax.experimental.pallas import tpu as pltpu
from jax.sharding import PartitionSpec as P

HD = 128
GROUP = 16
NEGATIVE = -1e30
EPSILON = 1e-06
REWARD_FLOOR = 0.25

Q_AT = (0, 3, 5, 3)
CORES = 2
CHUNKS = 4
STARTS = (0, 0, 5, 7)
PER_SLOT = 1
TILE = 800
PIECES = 5
WEIGH = 160
HALF = 8

BF16 = jnp.bfloat16
F32 = jnp.float32


def dot_last(a, b):
    return lax.dot_general(a, b, (((1,), (1,)), ((), ())), preferred_element_type=F32)


def send(src, dst, send_sem, recv_sem, device):
    return pltpu.make_async_remote_copy(
        src_ref=src,
        dst_ref=dst,
        send_sem=send_sem,
        recv_sem=recv_sem,
        device_id={"seq": device},
        device_id_type=pl.DeviceIdType.MESH,
    )


def kernel(
    dims,
    group_of,
    prompt_len,
    rewards,
    cont_len,
    groups,
    ids,
    gain,
    q,
    ck,
    cv,
    pk,
    pv,
    wt,
    lm,
    out,
    kvs,
    kvr,
    qs,
    qr,
    ab,
    hb,
    wv,
    gv,
    lv,
    smv,
    smg,
    run_f,
    run_m,
    run_s,
    run_p,
    st,
    sr,
    loc,
    kv_rs,
    kv_rd,
    kv_so,
    kv_sd,
    kv_su,
    kv_sn,
    q_rs,
    q_ss,
    sm_rs,
    sm_ss,
    g_rs,
    g_rd,
    g_sr,
    g_sl,
    g_sd,
    st_rs,
    st_ss,
):
    n, heads, per_head, conts, span, positions = dims
    chips = n // CORES
    side = chips // heads
    vocab = lm.shape[0]
    rows_q = conts * per_head * span
    one_q = per_head * span
    own = conts * span
    feats = wt.shape[0]
    width = per_head * HD
    chunk_rows = n // CHUNKS * own

    me = lax.axis_index("seq")
    z = lax.div(me, CORES)
    co = lax.rem(me, CORES)
    partner = me + 1 - 2 * co
    k0 = lax.div(z, side)
    j = lax.rem(z, side)
    base = k0 * side

    def chip(at):
        return lax.rem(at + chips, chips)

    def dev(at):
        return chip(at) * CORES + co

    barrier = pltpu.get_barrier_semaphore()

    def greet(d, carry):
        @pl.when(d != me)
        def _():
            pl.semaphore_signal(
                barrier, inc=1, device_id={"seq": d}, device_id_type=pl.DeviceIdType.MESH
            )

        return carry

    lax.fori_loop(0, n, greet, 0)

    def kv_loads(head):
        lanes = pl.ds(pl.multiple_of(head * HD, HD), HD)
        return lanes

    def load_kv(head, carry):
        lanes = kv_loads(head)
        pltpu.make_async_copy(pk.at[:, :, lanes], kvs.at[head, 0], loc.at[0]).start()
        pltpu.make_async_copy(pv.at[:, :, lanes], kvs.at[head, 1], loc.at[0]).start()
        return carry

    lax.fori_loop(0, heads, load_kv, 0)

    def load_q(head, carry):
        for a in range(conts):
            for g in range(per_head):
                lanes = pl.ds(pl.multiple_of((head * per_head + g) * HD, HD), HD)
                pltpu.make_async_copy(
                    q.at[a, :, lanes], qs.at[head, pl.ds(a * one_q + g * span, span), :], loc.at[1]
                ).start()
            lanes = pl.ds(pl.multiple_of(head * HD, HD), HD)
            pltpu.make_async_copy(
                ck.at[a, :, lanes], qs.at[head, pl.ds(rows_q + a * span, span), :], loc.at[1]
            ).start()
            pltpu.make_async_copy(
                cv.at[a, :, lanes], qs.at[head, pl.ds(rows_q + own + a * span, span), :], loc.at[1]
            ).start()
        return carry

    lax.fori_loop(0, heads, load_q, 0)

    lane = lax.broadcasted_iota(jnp.int32, (1, HD), 1)
    own_ids = ids[...].astype(F32)
    own_ids = jnp.concatenate([own_ids[a : a + 1, :] for a in range(conts)] * CORES, axis=1)
    own_ids = jnp.where(lax.div(lane, own) == co, own_ids, 0.0)
    own_rewards = jnp.zeros((1, HD), F32)
    for a in range(conts):
        own_rewards = jnp.where(lane == me * conts + a, rewards[a], own_rewards)
    smv[0:1, :] = own_ids
    smv[1:2, :] = own_rewards
    smg[me, 0:1, :] = own_ids
    smg[me, 1:2, :] = own_rewards

    with jax.named_scope("greet"):
        pltpu.make_async_copy(kvs, kvs, loc.at[0]).wait()
        pl.semaphore_wait(barrier, n - 1)

    def kv_at(src):
        rows = pl.ds(pl.multiple_of((chip(src) * CORES + co) * positions, positions), positions)
        return kvr.at[:, :, rows, :]

    def kv_sem(src):
        return chip(src)

    def kv_send(source, head_block, target, send_sem):
        return send(head_block, kv_at(source), send_sem, kv_rs.at[kv_sem(source)], dev(target))

    def kv_d2d(source, block):
        return send(
            block, kv_at(source), kv_sd.at[kv_sem(source)], kv_rd.at[kv_sem(source)], partner
        )

    next_head = lax.rem(k0 + 1, heads)
    prev_head = lax.rem(k0 + heads - 1, heads)
    far_head = lax.rem(k0 + 2, heads)
    own_right = kv_send(z, kvs.at[k0], z + 1, kv_so.at[0])
    own_left = kv_send(z, kvs.at[k0], z - 1, kv_so.at[1])
    ext_right = kv_send(z, kvs.at[next_head], base + side, kv_so.at[2])
    ext_left = kv_send(z, kvs.at[prev_head], base - 1, kv_so.at[3])
    far_right = kv_send(z, kvs.at[far_head], base + 2 * side, kv_so.at[4])
    far_left = kv_send(z, kvs.at[far_head], base - side - 1, kv_so.at[5])
    own_part = kv_d2d(z, kvs.at[k0])

    @pl.when(j < side - 1)
    def _():
        own_right.start()

    @pl.when(j > 0)
    def _():
        own_left.start()

    own_part.start()
    own_rows = pl.ds(pl.multiple_of(me * positions, positions), positions)
    own_lanes = pl.ds(pl.multiple_of(k0 * HD, HD), HD)
    keep_k = pltpu.make_async_copy(pk.at[:, :, own_lanes], kvr.at[0, :, own_rows, :], loc.at[3])
    keep_v = pltpu.make_async_copy(pv.at[:, :, own_lanes], kvr.at[1, :, own_rows, :], loc.at[4])
    keep_k.start()
    keep_v.start()

    pltpu.make_async_copy(qs, qs, loc.at[1]).wait()

    def q_send(step):
        target = chip(z + side * step)
        if 2 * step == heads:
            shifted = jnp.where(j >= side // 2, side * step - side // 2, side * step + side // 2)
            target = chip(z + shifted)
        return send(
            qs.at[lax.div(target, side)],
            qr.at[k0],
            q_ss.at[step],
            q_rs.at[k0],
            dev(target),
        )

    keep_q = []
    for a in range(conts):
        for g in range(per_head):
            lanes = pl.ds(pl.multiple_of((k0 * per_head + g) * HD, HD), HD)
            keep_q.append((q.at[a, :, lanes], pl.ds(a * one_q + g * span, span)))
        keep_q.append((ck.at[a, :, own_lanes], pl.ds(rows_q + a * span, span)))
        keep_q.append((cv.at[a, :, own_lanes], pl.ds(rows_q + own + a * span, span)))
    for source, rows in keep_q:
        pltpu.make_async_copy(source, qr.at[k0, rows, :], loc.at[5]).start()


    def small_send(d):
        return send(smv, smg.at[me], sm_ss.at[d], sm_rs.at[me], d)

    def small_out(d, carry):
        @pl.when(d != me)
        def _():
            small_send(d).start()

        return carry

    with jax.named_scope("small"):
        lax.fori_loop(0, n, small_out, 0)
    load_w = pltpu.make_async_copy(wt, wv, loc.at[6])
    load_w.start()
    load_lm = pltpu.make_async_copy(lm, lv.at[pl.ds(0, vocab), :], loc.at[2])
    load_lm.start()

    reach = side + side // 2

    def up_send(t):
        return kv_send(z - t, kv_at(z - t), z + 1, kv_su.at[t - 1])

    def down_send(t):
        return kv_send(z + t, kv_at(z + t), z - 1, kv_sn.at[t - 1])

    def depart(i):
        @pl.when(i == side - 1 - j)
        def _():
            ext_right.start()

        @pl.when(i == j)
        def _():
            ext_left.start()

        @pl.when(jnp.logical_and(j >= side // 2, i == 2 * (side - 1) - j))
        def _():
            far_right.start()

        @pl.when(jnp.logical_and(j < side // 2, i == side - 1 + j))
        def _():
            far_left.start()

        for step in range(1, heads):

            @pl.when(i == Q_AT[step])
            def _(step=step):
                q_send(step).start()

    def chain(i, carry):
        t = i + 1
        depart(i)

        @pl.when(t <= j + reach)
        def _():
            kv_send(z - t, kv_at(z - t), z + 1, kv_su.at[t - 1]).wait_recv()

            @pl.when(j < side - 1)
            def _():
                up_send(t).start()

            kv_d2d(z - t, kv_at(z - t)).start()

        @pl.when(t <= side - 1 - j + reach)
        def _():
            kv_send(z + t, kv_at(z + t), z - 1, kv_sn.at[t - 1]).wait_recv()

            @pl.when(j > 0)
            def _():
                down_send(t).start()

            kv_d2d(z + t, kv_at(z + t)).start()

        return carry

    longest = side - 1 + reach
    with jax.named_scope("chain"):
        lax.fori_loop(0, longest, chain, 0)

    keep_k.wait()
    keep_v.wait()
    pltpu.make_async_copy(qr.at[k0], qr.at[k0], loc.at[5]).wait()

    def other_rows(src):
        rows = pl.ds(
            pl.multiple_of((src * CORES + 1 - co) * positions, positions), positions
        )
        return kvr.at[:, :, rows, :]

    def kv_partner(src, carry):
        send(other_rows(src), other_rows(src), kv_sd.at[src], kv_rd.at[src], partner).wait_recv()
        return carry

    with jax.named_scope("kvpartner"):
        lax.fori_loop(0, chips, kv_partner, 0)

    def q_arrived(c, carry):
        @pl.when(c != k0)
        def _():
            send(qr.at[c], qr.at[c], q_ss.at[0], q_rs.at[c], partner).wait_recv()

        return carry

    with jax.named_scope("qarrive"):
        lax.fori_loop(0, heads, q_arrived, 0)

    def place_of(c, chip_id):
        k = lax.div(chip_id, side)
        away = lax.rem(c - k + heads, heads)
        place = lax.rem(chip_id, side)
        return jnp.where(2 * away == heads, lax.rem(place + side // 2, side), place)

    def token_row(c, chip_id, core):
        k = lax.div(chip_id, side)
        return ((k * side + place_of(c, chip_id)) * CORES + core) * own

    def block_at(stream, chip_id, core):
        d = chip(chip_id) * CORES + core
        if stream < CHUNKS:
            at = token_row(stream, chip(chip_id), core)
            return ab.at[stream, pl.ds(pl.multiple_of(at, own), own), :]
        return hb.at[stream - CHUNKS, pl.ds(pl.multiple_of(d * feats, 16), feats), :]

    def ring_send(stream, source, target, send_sem):
        block = block_at(stream, source, co)
        return send(block, block, send_sem, g_rs.at[stream, chip(source)], dev(target))

    def ring_right(stream, t):
        return ring_send(stream, z - t, z + 1, g_sr.at[stream, t])

    def ring_left(stream, t):
        return ring_send(stream, z + t, z - 1, g_sl.at[stream, t])

    def ring_d2d(stream, source):
        block = block_at(stream, source, co)
        return send(
            block, block, g_sd.at[stream, chip(source)], g_rd.at[stream, chip(source)], partner
        )

    def steps_of(stream):
        right = HALF if stream % 2 == 0 else chips - 1 - HALF
        return right, chips - 1 - right

    def ring_open(stream):
        ring_right(stream, 0).start()
        ring_left(stream, 0).start()
        ring_d2d(stream, z).start()

    def attended_open(c):
        rows = pl.ds(pl.multiple_of(token_row(c, z, co), own), own)
        block = ab.at[c, rows, :]
        send(block, block, g_sr.at[c, 0], g_rs.at[c, z], dev(z + 1)).start()
        send(block, block, g_sl.at[c, 0], g_rs.at[c, z], dev(z - 1)).start()
        send(block, block, g_sd.at[c, z], g_rd.at[c, z], partner).start()

    def ring_step(stream, t):
        right, left = steps_of(stream)

        @pl.when(t <= right)
        def _():
            ring_send(stream, z - t, z + 1, g_sr.at[stream, 0]).wait_recv()

            @pl.when(t < right)
            def _():
                ring_right(stream, t).start()

        @pl.when(t <= left)
        def _():
            ring_send(stream, z + t, z - 1, g_sl.at[stream, 0]).wait_recv()

            @pl.when(t < left)
            def _():
                ring_left(stream, t).start()

        @pl.when(t <= right)
        def _():
            ring_d2d(stream, z - t).start()

        @pl.when(t <= left)
        def _():
            ring_d2d(stream, z + t).start()

    def ring_partner(stream):
        def arrived(src, carry):
            block = block_at(stream, src, 1 - co)
            send(
                block, block, g_sd.at[stream, src], g_rd.at[stream, src], partner
            ).wait_recv()
            return carry

        lax.fori_loop(0, chips, arrived, 0)

    def attention(c):
        for a in range(conts):
            cont = ((c * side + place_of(c, z)) * CORES + co) * conts + a
            g = group_of[cont]
            length = prompt_len[g]
            queries = qr[c, pl.ds(a * one_q, one_q), :]
            own_keys = qr[c, pl.ds(rows_q + a * span, span), :]
            own_values = qr[c, pl.ds(rows_q + own + a * span, span), :]
            scores = dot_last(queries, kvr[0, g]) * HD ** (-0.5)
            at = lax.broadcasted_iota(jnp.int32, scores.shape, 1)
            scores = jnp.where(at < length, scores, NEGATIVE)
            near = dot_last(queries, own_keys) * HD ** (-0.5)
            token = lax.rem(lax.broadcasted_iota(jnp.int32, near.shape, 0), span)
            near = jnp.where(lax.broadcasted_iota(jnp.int32, near.shape, 1) <= token, near, NEGATIVE)
            peak = jnp.maximum(
                jnp.max(scores, axis=1, keepdims=True), jnp.max(near, axis=1, keepdims=True)
            )
            weights = jnp.exp(scores - peak)
            near = jnp.exp(near - peak)
            total = jnp.sum(weights, axis=1, keepdims=True) + jnp.sum(near, axis=1, keepdims=True)
            mixed = jnp.dot(weights.astype(BF16), kvr[1, g], preferred_element_type=F32)
            mixed += jnp.dot(near.astype(BF16), own_values, preferred_element_type=F32)
            mixed = (mixed / total).astype(BF16)
            rows = pl.ds(pl.multiple_of(token_row(c, z, co) + a * span, span), span)
            for g5 in range(per_head):
                ab[c, rows, g5 * HD : (g5 + 1) * HD] = mixed[g5 * span : (g5 + 1) * span, :]

    def project(c):
        total = jnp.zeros((feats, chunk_rows), F32)
        for k in range(heads):
            total += dot_last(
                wv[:, k * width : (k + 1) * width], ab[c, pl.ds(k * chunk_rows, chunk_rows), :]
            )
        hb[c, pl.ds(pl.multiple_of(me * feats, 16), feats), :] = total.astype(BF16)

    features = hb.shape[1]
    strip = HD

    def normalize(c):
        def squares(i, total):
            x = hb[c, pl.ds(pl.multiple_of(i * strip, strip), strip), :].astype(F32)
            return total + jnp.sum(x * x, axis=0, keepdims=True)

        total = lax.fori_loop(0, features // strip, squares, jnp.zeros((1, chunk_rows), F32))
        run_f[...] = lax.rsqrt(total / features + EPSILON)

    def weigh(i):
        rows = pl.ds(pl.multiple_of(i * WEIGH, 16), WEIGH)
        lv[rows, :] = (lv[rows, :].astype(F32) * gv[...]).astype(BF16)

    def chunk_ids(c):
        rows = []
        for i in range(side):
            d = (c * side + i) * CORES
            rows.append(smg[d, 0:1, :] + smg[d + 1, 0:1, :])
        ids = jnp.concatenate(rows, axis=1).astype(jnp.int32) - me * vocab
        return jnp.where(ids < vocab, ids, -1)

    def tile(c, v):
        ids_row = chunk_ids(c)
        part = TILE // PIECES
        peak, mass, hit = run_m[...], run_s[...], run_p[...]
        for piece in range(PIECES):
            first_row = v * TILE + piece * part
            rows = pl.ds(pl.multiple_of(first_row, 16), part)
            logits = jnp.dot(lv[rows, :], hb[c], preferred_element_type=F32) * run_f[...]
            at = lax.broadcasted_iota(jnp.int32, logits.shape, 0) + first_row
            logits = jnp.where(at < vocab, logits, NEGATIVE)
            hit += jnp.sum(jnp.where(at == ids_row, logits, 0.0), axis=0, keepdims=True)
            new = jnp.maximum(peak, jnp.max(logits, axis=0, keepdims=True))
            mass = mass * jnp.exp(peak - new) + jnp.sum(
                jnp.exp(logits - new), axis=0, keepdims=True
            )
            peak = new
        run_m[...] = peak
        run_s[...] = mass
        run_p[...] = hit

    def stats_send(c, i, core):
        d = (c * side + i) * CORES + core
        return d, send(st.at[c, i], sr.at[me], st_ss.at[d], st_rs.at[me], d)

    def stats_out(c):
        lse = run_m[...] + jnp.log(run_s[...])
        hit = run_p[...]
        for i in range(side):
            lanes = slice(i * HD, (i + 1) * HD)
            st[c, i, 0:1, :] = lse[:, lanes]
            st[c, i, 1:2, :] = hit[:, lanes]

        @pl.when(k0 == c)
        def _():
            own_lse, own_hit = lse[:, 0:HD], hit[:, 0:HD]
            for i in range(1, side):
                lanes = slice(i * HD, (i + 1) * HD)
                own_lse = jnp.where(j == i, lse[:, lanes], own_lse)
                own_hit = jnp.where(j == i, hit[:, lanes], own_hit)
            sr[me, 0:1, :] = own_lse
            sr[me, 1:2, :] = own_hit

        for i in range(side):
            for core in range(CORES):
                d, copy = stats_send(c, i, core)

                @pl.when(d != me)
                def _(copy=copy):
                    copy.start()

    tiles = -(-vocab // TILE)
    steps = []
    finished = 0
    while finished < tiles * CHUNKS:
        at = len(steps)
        steps.append(finished)
        ready = sum(at >= 2 * HALF + start for start in STARTS) * tiles
        finished = min(finished + PER_SLOT, ready)
    slots = len(steps)
    steps.append(finished)

    def slot(i, carry):
        for stream in range(CHUNKS):
            t = i - STARTS[stream]

            @pl.when(jnp.logical_and(t >= 1, t <= HALF))
            def _(stream=stream, t=t):
                with jax.named_scope(f"att{stream}"):
                    ring_step(stream, t)

        for stream in range(CHUNKS, 2 * CHUNKS):
            t = i - (STARTS[stream - CHUNKS] + HALF)

            @pl.when(jnp.logical_and(t >= 1, t <= HALF))
            def _(stream=stream, t=t):
                with jax.named_scope(f"hid{stream}"):
                    ring_step(stream, t)

        def begin(c, carry):
            with jax.named_scope("attention"):
                attention(c)
            attended_open(c)
            return carry

        begun = sum((i > start).astype(jnp.int32) for start in STARTS)
        due = sum((i >= start).astype(jnp.int32) for start in STARTS)
        lax.fori_loop(begun, due, begin, 0)

        @pl.when(i == HALF)
        def _():
            load_w.wait()

        @pl.when(i == 0)
        def _():
            load_lm.wait()
            for row in range(gain.shape[0]):
                gv[0:1, row * HD : (row + 1) * HD] = gain[row : row + 1, :]

        @pl.when(i < lv.shape[0] // WEIGH)
        def _():
            with jax.named_scope("weigh"):
                weigh(i)

        for c in range(CHUNKS):

            @pl.when(i == STARTS[c] + HALF)
            def _(c=c):
                with jax.named_scope("partner1"):
                    ring_partner(c)
                with jax.named_scope("project"):
                    project(c)
                ring_open(CHUNKS + c)

        m = i - 2 * HALF

        @pl.when(m == 0)
        def _():
            def small_in(d, carry):
                @pl.when(d != me)
                def _():
                    send(smg.at[d], smg.at[d], sm_ss.at[d], sm_rs.at[d], partner).wait_recv()

                return carry

            lax.fori_loop(0, n, small_in, 0)

        for c in range(CHUNKS):

            @pl.when(m == STARTS[c])
            def _(c=c):
                with jax.named_scope("partner2"):
                    ring_partner(CHUNKS + c)

        first = 0
        last = 0
        for at in range(2 * HALF, slots):
            first = first + jnp.where(i > at, steps[at + 1] - steps[at], 0)
            last = last + jnp.where(i >= at, steps[at + 1] - steps[at], 0)

        def one(step, carry):
            c = lax.div(step, tiles)
            v = lax.rem(step, tiles)

            @pl.when(v == 0)
            def _():
                with jax.named_scope("norm"):
                    normalize(c)
                run_m[...] = jnp.full_like(run_m, NEGATIVE)
                run_s[...] = jnp.zeros_like(run_s)
                run_p[...] = jnp.zeros_like(run_p)

            with jax.named_scope("tile"):
                tile(c, v)

            @pl.when(v == tiles - 1)
            def _():
                with jax.named_scope("stats"):
                    stats_out(c)

            return carry

        lax.fori_loop(first, last, one, 0)
        return carry

    with jax.named_scope("slots"):
        lax.fori_loop(0, slots, slot, 0)

    every_reward = jnp.sum(smg[...][:, 1, :], axis=0, keepdims=True)[:, 0 : n * conts]
    advantages = []
    for a in range(conts):
        same = groups[...] == group_of[me * conts + a]
        mean = jnp.sum(jnp.where(same, every_reward, 0.0), axis=1, keepdims=True) / GROUP
        off = every_reward - mean
        spread = jnp.sum(jnp.where(same, off * off, 0.0), axis=1, keepdims=True)
        spread = jnp.sqrt(spread / (GROUP - 1))
        advantages.append((rewards[a] - mean) / jnp.maximum(spread, REWARD_FLOOR))

    def stats_in(d, carry):
        @pl.when(d != me)
        def _():
            send(sr.at[d], sr.at[d], st_ss.at[d], st_rs.at[d], partner).wait_recv()

        return carry

    with jax.named_scope("join"):
        lax.fori_loop(0, n, stats_in, 0)
    everyone = sr[...]
    lse = everyone[:, 0, :]
    peak = jnp.max(lse, axis=0, keepdims=True)
    lse = peak + jnp.log(jnp.sum(jnp.exp(lse - peak), axis=0, keepdims=True))
    logprob = jnp.sum(everyone[:, 1, :], axis=0, keepdims=True) - lse
    logprob = jnp.where(co == 0, logprob[:, 0:own], logprob[:, own : 2 * own])
    position = lax.broadcasted_iota(jnp.int32, (1, span), 1)
    gains = jnp.zeros((1, HD), F32)
    objectives = jnp.zeros((1, HD), F32)
    for a in range(conts):
        live = jnp.where(position < cont_len[a], logprob[:, a * span : (a + 1) * span], 0.0)
        out[a : a + 1, 0:span] = live
        gained = advantages[a] * jnp.sum(live, axis=1, keepdims=True)
        gained = gained / jnp.full((1, 1), cont_len[a], jnp.int32).astype(F32)
        gains = jnp.where(lane == a, advantages[a], gains)
        objectives = jnp.where(lane == a, gained, objectives)
    out[conts : conts + 1, :] = gains
    out[conts + 1 : conts + 2, :] = objectives

    @pl.when(j >= side // 2)
    def _():
        far_right.wait_send()

    @pl.when(j < side // 2)
    def _():
        far_left.wait_send()

    ext_right.wait_send()
    ext_left.wait_send()

    @pl.when(j < side - 1)
    def _():
        own_right.wait_send()

    @pl.when(j > 0)
    def _():
        own_left.wait_send()

    own_part.wait_send()
    for step in range(1, heads):
        q_send(step).wait_send()

    def chain_out(i, carry):
        t = i + 1

        @pl.when(t <= j + reach)
        def _():
            @pl.when(j < side - 1)
            def _():
                up_send(t).wait_send()

            kv_d2d(z - t, kv_at(z - t)).wait_send()

        @pl.when(t <= side - 1 - j + reach)
        def _():
            @pl.when(j > 0)
            def _():
                down_send(t).wait_send()

            kv_d2d(z + t, kv_at(z + t)).wait_send()

        return carry

    lax.fori_loop(0, longest, chain_out, 0)

    def peers_out(d, carry):
        @pl.when(d != me)
        def _():
            small_send(d).wait_send()
            send(st.at[0, 0], sr.at[me], st_ss.at[d], st_rs.at[me], d).wait_send()

        return carry

    lax.fori_loop(0, n, peers_out, 0)

    def ring_out(t, carry):
        for stream in range(2 * CHUNKS):
            right, left = steps_of(stream)

            @pl.when(t < right)
            def _(stream=stream):
                ring_right(stream, t).wait_send()

            @pl.when(t < left)
            def _(stream=stream):
                ring_left(stream, t).wait_send()

            ring_d2d(stream, t).wait_send()
            ring_d2d(stream, t + HALF).wait_send()
        return carry

    lax.fori_loop(0, HALF, ring_out, 0)


def scores_of(
    n, group_of, prompt_len, rewards, cont_len, groups, ids, gain, q, ck, cv, pk, pv, wt, lm
):
    conts, span, query_width = q.shape
    prompts, positions, kv_width = pk.shape
    heads = kv_width // HD
    per_head = query_width // kv_width
    chips = n // CORES
    own = conts * span
    feats, features = wt.shape
    vocab = lm.shape[0]
    chunk_rows = n // CHUNKS * own
    chunk_q = own * per_head + 2 * own
    streams = 2 * CHUNKS
    side = chips // heads
    dims = (n, heads, per_head, conts, span, positions)
    dma = pltpu.SemaphoreType.DMA
    vmem_rows = -(-vocab // TILE) * TILE
    any_spec = pl.BlockSpec(memory_space=pl.ANY)
    smem_spec = pl.BlockSpec(memory_space=pltpu.SMEM)
    vmem_spec = pl.BlockSpec(memory_space=pltpu.VMEM)
    return pl.pallas_call(
        functools.partial(kernel, dims),
        out_shape=jax.ShapeDtypeStruct((8, HD), F32),
        in_specs=[smem_spec] * 4 + [vmem_spec] * 3 + [any_spec] * 7,
        out_specs=vmem_spec,
        scratch_shapes=[
            pltpu.VMEM((heads, 2, prompts, positions, HD), BF16),
            pltpu.VMEM((2, prompts, n * positions, HD), BF16),
            pltpu.VMEM((heads, chunk_q, HD), BF16),
            pltpu.VMEM((heads, chunk_q, HD), BF16),
            pltpu.VMEM((CHUNKS, n * own, per_head * HD), BF16),
            pltpu.VMEM((CHUNKS, n * feats, chunk_rows), BF16),
            pltpu.VMEM((feats, features), BF16),
            pltpu.VMEM((1, n * feats), F32),
            pltpu.VMEM((vmem_rows, n * feats), BF16),
            pltpu.VMEM((2, HD), F32),
            pltpu.VMEM((n, 2, HD), F32),
            pltpu.VMEM((1, chunk_rows), F32),
            pltpu.VMEM((1, chunk_rows), F32),
            pltpu.VMEM((1, chunk_rows), F32),
            pltpu.VMEM((1, chunk_rows), F32),
            pltpu.VMEM((CHUNKS, side, 2, HD), F32),
            pltpu.VMEM((n, 2, HD), F32),
            dma((9,)),
            dma((chips,)),
            dma((chips,)),
            dma((6,)),
            dma((chips,)),
            dma((chips,)),
            dma((chips,)),
            dma((heads,)),
            dma((heads,)),
            dma((n,)),
            dma((n,)),
            dma((streams, chips)),
            dma((streams, chips)),
            dma((streams, HALF)),
            dma((streams, HALF)),
            dma((streams, chips)),
            dma((n,)),
            dma((n,)),
        ],
        compiler_params=pltpu.CompilerParams(
            collective_id=0, has_side_effects=True, vmem_limit_bytes=67_043_328
        ),
        name="scores",
    )(group_of, prompt_len, rewards, cont_len, groups, ids, gain, q, ck, cv, pk, pv, wt, lm)


def per_device(
    n,
    cont_query,
    cont_key,
    cont_value,
    prefix_key,
    prefix_value,
    out_weight,
    norm_gain,
    lm_head,
    target_ids,
    cont_len,
    prompt_len,
    group_of,
    rewards,
):
    found = scores_of(
        n,
        group_of,
        prompt_len,
        rewards,
        cont_len,
        group_of.reshape(1, -1),
        target_ids,
        norm_gain.reshape(-1, HD),
        cont_query,
        cont_key,
        cont_value,
        prefix_key,
        prefix_value,
        out_weight.T,
        lm_head.T,
    )
    conts, span, _ = cont_query.shape
    return (found[:conts, :span], found[conts, :conts], found[conts + 1, :conts])


def solution(mesh):
    both = ("grp", "seq")
    in_specs = (
        P(both, None, None),
        P(both, None, None),
        P(both, None, None),
        P("grp", "seq", None),
        P("grp", "seq", None),
        P(None, "seq"),
        P(),
        P(None, "seq"),
        P(both, None),
        P(both),
        P("grp"),
        P("grp"),
        P(both),
    )
    out_specs = (P(both, None), P(both), P(both))
    return jax.shard_map(
        functools.partial(per_device, mesh.shape["seq"]),
        mesh=mesh,
        in_specs=in_specs,
        out_specs=out_specs,
        check_vma=False,
    )
```
